32 devices in a mesh: seq: 16 (over z, y, core), head: 2 (over x).
Axes of the slice: x: 2, y: 2, z: 4, core: 2. Of those that a mesh axis runs over, the one named last changes fastest.
Arguments:
- queries: bfloat16 [2048, 2048], P('seq', 'head'), may hold values from -190 to 190
- key_vectors: bfloat16 [2048, 256], P('seq', 'head'), may hold values from -6.1 to 6.1
- value_vectors: bfloat16 [2048, 256], P('seq', 'head'), may hold values from -54 to 54
- log_gate: float32 [16, 2048], P('head', 'seq'), may hold values from -1 to 0, as said below
- query_map: float32 [16, 128, 128], P('head'), may hold values from -0.5 to 0.5
- key_map: float32 [16, 128, 128], P('head'), may hold values from -0.5 to 0.5
- level_weight: float32 [16, 12], P('head'), may hold values from 0.25 to 2
- norm_gain: float32 [2048], P('head'), may hold values from 0.5 to 1.5
Outputs:
- grad_query_map: float32 [16, 128, 128], P('head')
- grad_key_map: float32 [16, 128, 128], P('head')
- grad_level_weight: float32 [16, 12], P('head')
- grad_norm_gain: float32 [2048], P('head')
The draws below stay inside these ranges and needn't reach their ends.
Inputs may be any that keep to these rules, and one draw needn't show every extreme that they name: `log_gate`: every entry is negative.
All inputs are finite; a program needn't handle non-finite values.
Results may differ from the reference program's by a relative error of at most 0.0015.
Values may be sent and summed in bfloat16 or wider, within the bound.
No kernel may reach another device: no remote copies, remote signals or barrier semaphores. Data moves between devices by JAX's collectives and lax.ppermute only.
A program may use at most 128 MiB of HBM per device.

```python
import math
import jax
import jax.numpy as jnp
from jax import lax

HD = 128
GROUP = 8
TOK_DEV = 128
KV_HEADS = 2
QUERY_HEAD_COUNT = 16
TOKENS = 2048
LEVELS = 12


def drawn_pair(key):
    base = jax.random.fold_in(key, 17)
    first, second = jax.random.split(base, 2)
    key_rows = jax.random.truncated_normal(first, -6.0, 6.0, (TOKENS, KV_HEADS, HD), jnp.float32)
    query_rows = jax.random.truncated_normal(second, -6.0, 6.0, (TOKENS, KV_HEADS, GROUP, HD), jnp.float32)
    return (query_rows.reshape(TOKENS, KV_HEADS * GROUP * HD), key_rows.reshape(TOKENS, KV_HEADS * HD))


def draw_queries(key, part):
    return drawn_pair(key)[0].astype(jnp.bfloat16)


def draw_key_vectors(key, part):
    return drawn_pair(key)[1].astype(jnp.bfloat16)


def draw_value_vectors(key, part):
    base = jax.random.fold_in(key, 23)
    value_rows = jax.random.truncated_normal(base, -6.0, 6.0, (TOKENS, KV_HEADS, HD), jnp.float32)
    ramp = jnp.arange(KV_HEADS).astype(jnp.float32) / max(KV_HEADS - 1, 1)
    head_scale = 1.0 + 2.0 * ramp
    return (value_rows * head_scale[None, :, None]).reshape(TOKENS, KV_HEADS * HD).astype(jnp.bfloat16)


def draw_log_gate(key, part):
    base = jax.random.fold_in(key, 31)
    component_listing = jax.random.split(base, 7)
    head_draw = jax.random.uniform(component_listing[0], (QUERY_HEAD_COUNT,), jnp.float32)
    fast_share = 0.5
    is_fast = head_draw < fast_share
    fast_rate = jnp.exp(jax.random.uniform(component_listing[1], (QUERY_HEAD_COUNT,), jnp.float32, math.log(1.0 / 50.0), math.log(1.0 / 30.0)))
    slow_rate = jnp.exp(jax.random.uniform(component_listing[2], (QUERY_HEAD_COUNT,), jnp.float32, math.log(0.2), math.log(0.6))) / TOKENS
    head_frequency = jnp.where(is_fast, fast_rate, slow_rate)
    extent_multiplier = jnp.exp(jax.random.uniform(component_listing[3], (QUERY_HEAD_COUNT, TOKENS // TOK_DEV), jnp.float32, math.log(0.5), math.log(2.0)))
    extent_multiplier = jnp.repeat(extent_multiplier, TOK_DEV, axis=1)
    jaggedness = jax.random.uniform(component_listing[4], (QUERY_HEAD_COUNT, TOKENS), jnp.float32, 0.5, 1.5)
    spots = jax.random.randint(component_listing[5], (3,), 0, TOKENS)
    cluster_depth = jax.random.uniform(component_listing[6], (3, QUERY_HEAD_COUNT), jnp.float32, 0.22, 0.4)
    positions = jnp.arange(TOKENS)
    match_total = (positions[None, :] == spots[:, None]).astype(jnp.float32)
    clusters_drawn = jnp.einsum('mv,ml->vl', cluster_depth, match_total)
    return -(head_frequency[:, None] * extent_multiplier * jaggedness) - clusters_drawn


def levels(rng, extent, cuts, low, high):
    loudness = 1.0
    for dim, shards_of in cuts:
        heights = jax.random.uniform(jax.random.fold_in(jax.random.fold_in(rng, 6), dim), (shards_of,), jnp.float32, low / len(cuts), high / len(cuts))
        loudness = loudness * jnp.repeat(jnp.exp(heights), extent[dim] // shards_of).reshape((-1,) + (1,) * (len(extent) - 1 - dim))
    return loudness


def gaussian(own_key, extent, deviation, bound, cuts=(), held_as=jnp.bfloat16):
    factor_of = levels(own_key, extent, cuts, -0.22, 0.18) if cuts else 1.0
    result = jax.random.normal(own_key, extent, jnp.float32) * deviation * factor_of
    return jnp.minimum(jnp.maximum(result, -bound), bound).astype(held_as)


def setup_inputs(seed: int = 0) -> dict:
    keys = jax.random.split(jax.random.key(seed), 9)
    return {
        "queries": draw_queries(jax.random.fold_in(keys[8], 71), 0),
        "key_vectors": draw_key_vectors(jax.random.fold_in(keys[8], 71), 0),
        "value_vectors": draw_value_vectors(jax.random.fold_in(keys[8], 71), 0),
        "log_gate": draw_log_gate(jax.random.fold_in(keys[8], 71), 0),
        "query_map": gaussian(keys[4], (QUERY_HEAD_COUNT, HD, HD), HD ** -0.5, 0.5, ((0, 2),), jnp.float32),
        "key_map": gaussian(keys[5], (QUERY_HEAD_COUNT, HD, HD), HD ** -0.5, 0.5, ((0, 2),), jnp.float32),
        "level_weight": jnp.clip(jnp.exp(math.log(2.0) - 2.0794415 * jax.random.uniform(keys[6], (QUERY_HEAD_COUNT, LEVELS), jnp.float32) ** levels(keys[6], (QUERY_HEAD_COUNT, LEVELS), ((0, 2),), -0.2, 0.2)), 0.25, 2.0),
        "norm_gain": jnp.clip(1.0 + 0.1 * jax.random.normal(keys[7], (QUERY_HEAD_COUNT * HD,), jnp.float32), 0.5, 1.5),
    }


HIGHEST = lax.Precision.HIGHEST
EPSILON = 1e-05

def bit_length(numbers, bit_count):
    digits = jnp.zeros_like(numbers)
    for bit_power in range(bit_count):
        digits = digits + (numbers >= 1 << bit_power).astype(jnp.int32)
    return digits

def teacher(query_rows, key_rows, value_rows):
    score_scale = HD ** (-0.5)
    positions = jnp.arange(TOKENS, dtype=jnp.int32)
    keys_float = key_rows.astype(jnp.float32)
    values_float = value_rows.astype(jnp.float32)

    def block_out(block_id):
        block_rows = lax.dynamic_slice_in_dim(query_rows, block_id * TOK_DEV, TOK_DEV, 0).astype(jnp.float32)
        scores = jnp.einsum('rgd,kd->grk', block_rows, keys_float, precision=HIGHEST) * score_scale
        own_pos = block_id * TOK_DEV + jnp.arange(TOK_DEV, dtype=jnp.int32)
        scores = jnp.where(positions[None, None, :] <= own_pos[None, :, None], scores, -jnp.inf)
        row_peak = lax.optimization_barrier(jnp.max(scores, axis=2, keepdims=True))
        weights = jnp.exp(scores - row_peak)
        rounded = lax.optimization_barrier(weights.astype(jnp.bfloat16)).astype(jnp.float32)
        weighted = jnp.einsum('grk,kd->grd', rounded, values_float, precision=HIGHEST)
        return weighted / lax.optimization_barrier(jnp.sum(weights, axis=2))[..., None]
    block_outs = lax.map(block_out, jnp.arange(TOKENS // TOK_DEV, dtype=jnp.int32))
    return block_outs.transpose(1, 0, 2, 3).reshape(GROUP, TOKENS, HD)

def student(query_maps, key_maps, level_rows, query_rows, key_rows, value_rows, gate_rows):
    span_total = TOKENS // TOK_DEV
    low_bits = TOK_DEV.bit_length() - 1
    query_float = query_rows.astype(jnp.float32)
    keys_float = key_rows.astype(jnp.float32)
    values_float = value_rows.astype(jnp.float32)
    query_proj = jnp.einsum('tgd,gde->gte', query_float, query_maps, precision=HIGHEST).reshape(GROUP, span_total, TOK_DEV, HD)
    key_proj = jnp.einsum('td,gde->gte', keys_float, key_maps, precision=HIGHEST).reshape(GROUP, span_total, TOK_DEV, HD)
    values_spans = values_float.reshape(span_total, TOK_DEV, HD)
    keys_spans = keys_float.reshape(span_total, TOK_DEV, HD)
    cumulative = jnp.cumsum(gate_rows, axis=1).reshape(GROUP, span_total, TOK_DEV)
    position = jnp.arange(TOK_DEV, dtype=jnp.int32)
    causal = position[None, :] <= position[:, None]
    level_ids = jnp.arange(LEVELS, dtype=jnp.int32)
    local_level = bit_length(jnp.bitwise_xor(position[:, None], position[None, :]), LEVELS)
    local_pick = (local_level[None] == level_ids[:, None, None]).astype(jnp.float32)
    level_mask = jnp.einsum('gl,lrs->grs', level_rows, local_pick, precision=HIGHEST)
    decay_in = jnp.exp(jnp.where(causal[None, None], cumulative[..., :, None] - cumulative[..., None, :], -jnp.inf))
    scores = jnp.einsum('gcre,gcse->gcrs', query_proj, key_proj, precision=HIGHEST)
    local_part = jnp.einsum('gcrs,csd->gcrd', scores * decay_in * level_mask[:, None], values_spans, precision=HIGHEST)
    ending = cumulative[:, :, -1]
    before = jnp.concatenate([jnp.zeros((GROUP, 1), ending.dtype), ending[:, :-1]], axis=1)
    raw_state = jnp.einsum('gcs,csa,csb->gcab', jnp.exp(ending[..., None] - cumulative), keys_spans, values_spans, precision=HIGHEST)
    span_ids = jnp.arange(span_total, dtype=jnp.int32)
    span_level = low_bits + bit_length(jnp.bitwise_xor(span_ids[:, None], span_ids[None, :]), LEVELS)
    span_pick = (span_level[None] == level_ids[:, None, None]).astype(jnp.float32)
    earlier = span_ids[None, :] < span_ids[:, None]
    link_decay = jnp.exp(jnp.where(earlier[None], before[:, :, None] - ending[:, None, :], -jnp.inf))
    coupling = link_decay * jnp.einsum('gl,lcx->gcx', level_rows, span_pick, precision=HIGHEST)
    combined = jnp.einsum('gcx,gxab->gcab', coupling, raw_state, precision=HIGHEST)
    key_state = jnp.einsum('gba,gcbf->gcaf', key_maps, combined, precision=HIGHEST)
    entry_decay = jnp.exp(cumulative - before[..., None])
    far_part = entry_decay[..., None] * jnp.einsum('gcre,gcef->gcrf', query_proj, key_state, precision=HIGHEST)
    return (local_part + far_part).reshape(GROUP, TOKENS, HD)

def reference(queries, key_vectors, value_vectors, log_gate, query_map, key_map, level_weight, norm_gain):
    query_rows = queries.reshape(TOKENS, KV_HEADS, GROUP, HD).transpose(1, 0, 2, 3)
    key_rows = key_vectors.reshape(TOKENS, KV_HEADS, HD).transpose(1, 0, 2)
    value_rows = value_vectors.reshape(TOKENS, KV_HEADS, HD).transpose(1, 0, 2)
    gate_rows = log_gate.reshape(KV_HEADS, GROUP, TOKENS)
    target = lax.map(lambda head_items: teacher(*head_items), (query_rows, key_rows, value_rows))
    checked = jax.checkpoint(student)

    def distill_loss(parameters):
        query_maps, key_maps, level_rows, gain_rows = parameters
        head_outs = lax.map(lambda head_items: checked(*head_items), (query_maps.reshape(KV_HEADS, GROUP, HD, HD), key_maps.reshape(KV_HEADS, GROUP, HD, HD), level_rows.reshape(KV_HEADS, GROUP, LEVELS), query_rows, key_rows, value_rows, gate_rows))
        square_sum = lax.optimization_barrier(jnp.sum(head_outs * head_outs, axis=(0, 1, 3)))
        inverse = lax.rsqrt(square_sum / (QUERY_HEAD_COUNT * HD) + EPSILON)
        normed = head_outs * inverse[None, None, :, None]
        student_out = normed * gain_rows.reshape(KV_HEADS, GROUP, 1, HD)
        mismatch = student_out - target
        return jnp.sum(mismatch * mismatch) / (2.0 * TOKENS)
    grad_query, grad_key, grad_levels, grad_gain = jax.grad(distill_loss)((query_map, key_map, level_weight, norm_gain))
    return (grad_query, grad_key, grad_levels, grad_gain)
```

```python
import functools

import jax
import jax.numpy as jnp
from jax import lax
from jax.experimental import pallas as pl
from jax.experimental.pallas import tpu as pltpu
from jax.sharding import PartitionSpec as P

HIGHEST = lax.Precision.HIGHEST
NEGATIVE = -1e30
EPSILON = 1e-05
F32 = jnp.float32
BF16 = jnp.bfloat16
NN = (((1,), (0,)), ((), ()))
NT = (((1,), (1,)), ((), ()))
TN = (((0,), (0,)), ((), ()))
GATE_ROWS = 32


def dot(a, b, dims=NN):
    return lax.dot_general(a, b, dims, preferred_element_type=F32)


def exact_dot(a, b, dims=NN):
    return lax.dot_general(a, b, dims, precision=HIGHEST, preferred_element_type=F32)


def halves(x):
    high = x.astype(BF16)
    return high, (x - high.astype(F32)).astype(BF16)


def dot_f32(a, b, dims=NN):
    lhs = jnp.concatenate([a[0], a[0], a[1]], axis=dims[0][0][0])
    rhs = jnp.concatenate([b[0], b[1], b[0]], axis=dims[0][1][0])
    return dot(lhs, rhs, dims)


def dot_left(a, b, dims=NN):
    lhs = jnp.concatenate([a[0], a[1]], axis=dims[0][0][0])
    rhs = jnp.concatenate([b, b], axis=dims[0][1][0])
    return dot(lhs, rhs, dims)


def dot_right(a, b, dims=NN):
    lhs = jnp.concatenate([a, a], axis=dims[0][0][0])
    rhs = jnp.concatenate([b[0], b[1]], axis=dims[0][1][0])
    return dot(lhs, rhs, dims)


def iota2(shape, axis):
    return lax.broadcasted_iota(jnp.int32, shape, axis)


def upper_ones(size):
    return (iota2((size, size), 0) <= iota2((size, size), 1)).astype(F32)


def slot_offset(position, strides):
    offset = position * 0
    for bit, stride in enumerate(strides):
        offset = offset + ((position >> bit) & 1) * stride
    return offset


def pack_kernel(k_ref, v_ref, gate_ref, out_ref):
    rows = k_ref.shape[0]
    heads = gate_ref.shape[0]
    out_ref[0:rows, :] = k_ref[...].astype(F32).T.astype(BF16)
    out_ref[rows : 2 * rows, :] = v_ref[...]
    gate = gate_ref[...]
    high = gate.astype(BF16).astype(F32)
    middle = (gate - high).astype(BF16).astype(F32)
    low = gate - high - middle
    blank = jnp.zeros((GATE_ROWS - 3 * heads, gate.shape[1]), F32)
    out_ref[2 * rows :, :] = jnp.concatenate([high, middle, low, blank], axis=0).astype(BF16)


def local_kernel(level_ref, gate_ref, q_ref, kt_ref, v_ref, qmap_ref, kmap_ref, qp_ref, qt_ref, sd_ref, mix_ref, loc_ref):
    heads, rows = gate_ref.shape
    dim = v_ref.shape[1]
    low_bits = rows.bit_length() - 1
    cum = exact_dot(gate_ref[...], upper_ones(rows))
    cum_t = cum.T
    row, col = iota2((rows, rows), 0), iota2((rows, rows), 1)
    causal = col <= row
    differ = row ^ col
    kt = kt_ref[...]
    v = v_ref[...]
    for h in range(heads):
        q = q_ref[:, h * dim : (h + 1) * dim]
        qp = dot_right(q, halves(qmap_ref[h]))
        qp_ref[h] = qp
        qt = dot_f32(halves(qp), halves(kmap_ref[h]), NT)
        qt_ref[h] = qt
        score = dot_left(halves(qt), kt)
        decay = jnp.exp(jnp.where(causal, cum_t[:, h : h + 1] - cum[h : h + 1, :], NEGATIVE))
        weight = jnp.full((rows, rows), level_ref[h, 0], F32)
        for level in range(1, low_bits + 1):
            weight = jnp.where(differ >= (1 << (level - 1)), level_ref[h, level], weight)
        mix = decay * weight
        mix_ref[h] = mix
        sd_ref[h] = score * decay
        loc_ref[h] = dot_left(halves(score * mix), v)


def forward_kernel(
    span_ref, level_ref, q_ref, even_ref, odd_ref, qt_ref, loc_ref, gain_ref,
    raw_ref, target_ref, state_ref, comb_ref, sums_ref,
    score_scr, peak_scr, total_scr, acc_scr, gate_scr, *, strides,
):
    heads, rows, dim = qt_ref.shape
    half = even_ref.shape[0]
    span_bits = state_ref.shape[0]
    low_bits = rows.bit_length() - 1
    span = span_ref[0]
    scale = dim ** (-0.5)
    total_rows = 2 * half * heads

    gates = []
    for ref in (even_ref, odd_ref):
        for p in range(half):
            piece = ref[p, 2 * rows : 2 * rows + GATE_ROWS, :].astype(F32)
            gates.append(piece[0:heads] + piece[heads : 2 * heads] + piece[2 * heads : 3 * heads])
    cum = exact_dot(jnp.concatenate(gates, axis=0), upper_ones(rows))
    ends = jnp.broadcast_to(cum[:, rows - 1 : rows], (total_rows, rows))

    def span_of(index):
        slot = index // heads
        return span ^ (slot_offset(slot % half, strides) + slot // half), index % heads

    mine, my_head = span_of(iota2((total_rows, total_rows), 0))
    other, other_head = span_of(iota2((total_rows, total_rows), 1))
    between = (other > mine) & (other < span) & (my_head == other_head)
    carried = exact_dot(between.astype(F32), ends)
    decay = jnp.exp(carried + ends - cum)
    for slot in range(2 * half):
        gate_scr[slot] = decay[slot * heads : (slot + 1) * heads]

    q_all = jnp.concatenate([q_ref[:, h * dim : (h + 1) * dim] for h in range(heads)], axis=0)
    row, col = iota2((rows, rows), 0), iota2((rows, rows), 1)
    causal = jnp.concatenate([col <= row] * heads, axis=0)
    score = jnp.where(causal, dot(q_all, even_ref[0, 0:rows, :]) * scale, NEGATIVE)
    score_scr[0] = score
    peak_scr[...] = score
    state_ref[...] = jnp.zeros_like(state_ref)

    def first_pass(p, carry):
        for parity, ref in ((0, even_ref), (1, odd_ref)):
            offset = slot_offset(p, strides) + parity
            slot = p + parity * half

            @pl.when((span ^ offset) < span)
            def _(ref=ref, offset=offset, slot=slot):
                kt = ref[p, 0:rows, :]
                v = ref[p, rows : 2 * rows, :]
                s = dot(q_all, kt) * scale
                score_scr[slot] = s
                peak_scr[...] = jnp.maximum(peak_scr[...], s)
                level = jnp.int32(-1)
                for bit in range(span_bits):
                    level = level + (offset >= (1 << bit)).astype(jnp.int32)
                kt32 = kt.astype(F32)
                w = gate_scr[slot]
                for h in range(heads):
                    state_ref[level, h] += dot_left(halves(kt32 * w[h : h + 1, :]), v)

        return carry

    lax.fori_loop(0, half, first_pass, 0)
    peak = jnp.max(peak_scr[...], axis=1, keepdims=True)
    peak_scr[...] = jnp.broadcast_to(peak, peak_scr.shape)
    total_scr[...] = jnp.zeros_like(total_scr)
    acc_scr[...] = jnp.zeros_like(acc_scr)

    def second_pass(p, carry):
        for parity, ref in ((0, even_ref), (1, odd_ref)):
            offset = slot_offset(p, strides) + parity
            slot = p + parity * half

            @pl.when((span ^ offset) <= span)
            def _(ref=ref, slot=slot):
                weight = jnp.exp(score_scr[slot] - peak_scr[...])
                total_scr[...] += weight
                acc_scr[...] += dot(weight.astype(BF16), ref[p, rows : 2 * rows, :])

        return carry

    lax.fori_loop(0, half, second_pass, 0)
    total = jnp.sum(total_scr[...], axis=1, keepdims=True)
    target_all = acc_scr[...] / total

    own = cum[0:heads]
    entry = jnp.exp(own.T)
    squares = jnp.zeros((rows, dim), F32)
    gained = jnp.zeros((rows, dim), F32)
    crossed = jnp.zeros((rows, dim), F32)
    for h in range(heads):
        combined = jnp.zeros((dim, dim), F32)
        for level in range(span_bits):
            combined = combined + level_ref[h, low_bits + 1 + level] * state_ref[level, h]
        comb_ref[h] = combined
        far = entry[:, h : h + 1] * dot_f32(halves(qt_ref[h]), halves(combined))
        raw = loc_ref[h] + far
        target = target_all[h * rows : (h + 1) * rows]
        raw_ref[h] = raw
        target_ref[h] = target
        gain = gain_ref[h : h + 1, :]
        square = raw * raw
        squares = squares + square
        gained = gained + square * (gain * gain)
        crossed = crossed + target * raw * gain
    lanes = iota2((rows, rows), 1)
    columns = jnp.where(
        lanes == 0,
        jnp.sum(squares, axis=1, keepdims=True),
        jnp.where(
            lanes == 1,
            jnp.sum(gained, axis=1, keepdims=True),
            jnp.where(lanes == 2, jnp.sum(crossed, axis=1, keepdims=True), 0.0),
        ),
    )
    sums_ref[...] = columns.T[0:8]


def backward_kernel(
    span_ref, sums_a_ref, sums_b_ref, gate_ref, q_ref, k_ref, v_ref, kmap_ref, gain_ref,
    qp_ref, qt_ref, sd_ref, mix_ref, raw_ref, target_ref, state_ref, comb_ref,
    keep_ref, send_ref, *, norm_width, total_tokens, splits,
):
    heads, rows, dim = qt_ref.shape
    span_bits = state_ref.shape[0]
    low_bits = rows.bit_length() - 1
    span = span_ref[0]
    parity = span & 1
    sums = (sums_a_ref[...] + sums_b_ref[...]).T
    squares, gained, crossed = sums[:, 0:1], sums[:, 1:2], sums[:, 2:3]
    inverse = lax.rsqrt(squares / norm_width + EPSILON)
    inner = (inverse * gained - crossed) / total_tokens
    shrink = inverse * inverse * inverse * inner / norm_width
    entry = jnp.exp(exact_dot(gate_ref[...], upper_ones(rows)).T)
    k = k_ref[...]
    v = v_ref[...]
    row, col = iota2((rows, rows), 0), iota2((rows, rows), 1)
    differ = row ^ col
    levels = low_bits + 1 + span_bits
    pad = 16
    level_rows = []
    gain_rows = []
    group = heads // (1 << len(splits))
    for h in range(heads):
        gain = gain_ref[h : h + 1, :]
        raw = raw_ref[h]
        normed = raw * inverse
        mismatch = (normed * gain - target_ref[h]) / total_tokens
        gain_rows.append(jnp.sum(mismatch * normed, axis=0, keepdims=True))
        residual = inverse * (mismatch * gain) - raw * shrink
        r_half = halves(residual)
        d_mix = dot_left(r_half, v, NT)
        d_score = d_mix * mix_ref[h]
        through = d_mix * sd_ref[h]
        lead = entry[:, h : h + 1] * residual
        lead_half = halves(lead)
        comb_half = halves(comb_ref[h])
        d_qt = dot_left(halves(d_score), k) + dot_f32(lead_half, comb_half, NT)
        d_qt_half = halves(d_qt)
        grad_k = dot_f32(d_qt_half, halves(qp_ref[h]), TN)
        d_qp = dot_f32(d_qt_half, halves(kmap_ref[h]))
        grad_q = dot_right(q_ref[:, h * dim : (h + 1) * dim], halves(d_qp), TN)
        d_comb = dot_f32(halves(qt_ref[h]), lead_half, TN)
        for level in range(low_bits + 1):
            low = 0 if level == 0 else 1 << (level - 1)
            high = 1 << level
            level_rows.append(
                jnp.sum(jnp.where((differ >= low) & (differ < high), through, 0.0), axis=0, keepdims=True)
            )
        for level in range(span_bits):
            level_rows.append(jnp.sum(state_ref[level, h] * d_comb, axis=0, keepdims=True))
        level_rows.append(jnp.zeros((pad - levels, rows), F32))
        chunk = 0
        for place, stride in enumerate(splits):
            bit = (h // group >> (len(splits) - 1 - place)) & 1
            mine = (span // stride) & 1
            chunk = chunk + ((bit ^ mine) << (len(splits) - 1 - place))
        at = pl.ds(pl.multiple_of((chunk * group + h % group) * dim, dim), dim)
        first = parity == 0
        keep_ref[at, :] = jnp.where(first, grad_q, grad_k)
        send_ref[at, :] = jnp.where(first, grad_k, grad_q)
    table = jnp.sum(jnp.concatenate(level_rows, axis=0), axis=1, keepdims=True)
    spread = iota2((heads * pad, rows), 0) % pad == iota2((heads * pad, rows), 1)
    pick = iota2((heads, heads * pad), 1) // pad == iota2((heads, heads * pad), 0)
    level_sums = exact_dot(pick.astype(F32), jnp.where(spread, table, 0.0))
    small = jnp.concatenate(gain_rows + [level_sums], axis=0)
    tail = pl.ds(heads * dim, 2 * heads)
    keep_ref[tail, :] = small
    send_ref[tail, :] = small


def place_kernel(span_ref, mine_ref, other_ref, q_ref, k_ref, *, splits):
    heads, dim, width = q_ref.shape
    span = span_ref[0]
    first = (span & 1) == 0
    group = heads // (1 << len(splits))
    for h in range(heads):
        chunk = 0
        for place, stride in enumerate(splits):
            bit = (h // group >> (len(splits) - 1 - place)) & 1
            mine = (span // stride) & 1
            chunk = chunk + ((bit ^ mine) << (len(splits) - 1 - place))
        at = pl.ds(pl.multiple_of((chunk * group + h % group) * dim, dim), dim)
        mine, other = mine_ref[at, :], other_ref[at, :]
        q_ref[h] = jnp.where(first, mine, other)
        k_ref[h] = jnp.where(first, other, mine)


def vmem(count):
    return [pl.BlockSpec(memory_space=pltpu.VMEM)] * count


def smem(count):
    return [pl.BlockSpec(memory_space=pltpu.SMEM)] * count


def shape(*dims, dtype=F32):
    return jax.ShapeDtypeStruct(dims, dtype)


def call(kernel, ins, outs, limit, flops, scratch=(), **static):
    body = functools.partial(kernel, **static) if static else kernel
    single = not isinstance(outs, (list, tuple))
    return pl.pallas_call(
        body,
        out_shape=outs,
        in_specs=ins,
        out_specs=pl.BlockSpec(memory_space=pltpu.VMEM) if single else vmem(len(outs)),
        scratch_shapes=list(scratch),
        compiler_params=pltpu.CompilerParams(vmem_limit_bytes=limit << 20),
        cost_estimate=pl.CostEstimate(flops=flops, bytes_accessed=1 << 20, transcendentals=0),
        name=kernel.__name__,
    )


def swap(value, axis, stride):
    count = lax.axis_size(axis)
    return lax.ppermute(value, axis, [(i, i ^ stride) for i in range(count)])


def on_device(queries, key_vectors, value_vectors, log_gate, query_map, key_map, level_weight, norm_gain):
    rows, dim = key_vectors.shape
    heads = queries.shape[1] // dim
    count = lax.axis_size("seq")
    groups = lax.axis_size("head")
    span_bits = count.bit_length() - 1
    span = lax.axis_index("seq").astype(jnp.int32).reshape(1)
    total_tokens = rows * count
    norm_width = heads * dim * groups
    gain = norm_gain.reshape(heads, dim)
    strides = [1 << bit for bit in reversed(range(1, span_bits))]
    splits = (2, 4)
    cube = (heads, dim, dim)
    packed_rows = 2 * rows + GATE_ROWS

    packed = call(pack_kernel, vmem(3), shape(packed_rows, rows, dtype=BF16), 8, 1 << 20)(
        key_vectors, value_vectors, log_gate
    )
    qp, qt, score_decay, mix, local = call(
        local_kernel, smem(1) + vmem(6), [shape(*cube)] * 5, 24, 1 << 29
    )(level_weight, log_gate, queries, packed[0:rows], value_vectors, query_map, key_map)

    even = packed[None]
    for stride in strides:
        even = jnp.concatenate([even, swap(even, "seq", stride)], axis=0)
    odd = swap(even, "seq", 1)

    raw, target, states, combined, sums = call(
        forward_kernel,
        smem(2) + vmem(6),
        [shape(*cube), shape(*cube), shape(span_bits, *cube), shape(*cube), shape(8, rows)],
        44,
        1 << 31,
        scratch=[
            pltpu.VMEM((count, heads * rows, rows), F32),
            pltpu.VMEM((heads * rows, rows), F32),
            pltpu.VMEM((heads * rows, rows), F32),
            pltpu.VMEM((heads * rows, dim), F32),
            pltpu.VMEM((count, heads, rows), F32),
        ],
        strides=tuple(strides),
    )(span, level_weight, queries, even, odd, qt, local, gain)

    stride = 1
    while stride < groups:
        received = swap(sums, "head", stride)
        if 2 * stride < groups:
            sums = sums + received
        stride *= 2

    keep, send = call(
        backward_kernel,
        smem(1) + vmem(16),
        [shape(heads * (dim + 2), dim)] * 2,
        32,
        1 << 30,
        norm_width=float(norm_width),
        total_tokens=float(total_tokens),
        splits=splits,
    )(
        span, sums, received, log_gate, queries, key_vectors, value_vectors, key_map, gain,
        qp, qt, score_decay, mix, raw, target, states, combined,
    )

    held = keep + swap(send, "seq", 1)
    size = heads * dim
    for split in splits:
        size //= 2
        received = swap(held[size:], "seq", split)
        held = jnp.concatenate([held[:size] + received[:size], held[2 * size :] + received[size:]])
    for stride in strides:
        if stride not in splits:
            held = held + swap(held, "seq", stride)
    small = held[size:]
    mine = held[:size]
    for split in reversed(splits):
        mine = jnp.concatenate([mine, swap(mine, "seq", split)])
    other = swap(mine, "seq", 1)
    grad_query, grad_key = call(place_kernel, smem(1) + vmem(2), [shape(*cube)] * 2, 16, 1 << 20, splits=splits)(
        span, mine, other
    )
    grad_gain = small[:heads].reshape(-1)
    grad_levels = small[heads:, : level_weight.shape[1]]
    return grad_query, grad_key, grad_levels, grad_gain


def solution(mesh):
    placed = (
        P("seq", "head"),
        P("seq", "head"),
        P("seq", "head"),
        P("head", "seq"),
        P("head", None, None),
        P("head", None, None),
        P("head", None),
        P("head"),
    )
    return jax.shard_map(
        on_device,
        mesh=mesh,
        in_specs=placed,
        out_specs=(P("head", None, None), P("head", None, None), P("head", None), P("head")),
        check_vma=False,
    )
```

```python
import functools

import jax
import jax.numpy as jnp
from jax import lax
from jax.experimental import pallas as pl
from jax.experimental.pallas import tpu as pltpu
from jax.sharding import PartitionSpec as P


HIGHEST = lax.Precision.HIGHEST
NEGATIVE = -1e30
EPSILON = 1e-05
F32 = jnp.float32
BF16 = jnp.bfloat16
NN = (((1,), (0,)), ((), ()))
NT = (((1,), (1,)), ((), ()))
TN = (((0,), (0,)), ((), ()))
GATE_ROWS = 32
PARTS = 2


def dot(a, b, dims=NN):
    return lax.dot_general(a, b, dims, preferred_element_type=F32)


def exact_dot(a, b, dims=NN):
    return lax.dot_general(a, b, dims, precision=HIGHEST, preferred_element_type=F32)


def halves(x):
    high = x.astype(BF16)
    return high, (x - high.astype(F32)).astype(BF16)


def dot_f32(a, b, dims=NN):
    lhs = jnp.concatenate([a[0], a[0], a[1]], axis=dims[0][0][0])
    rhs = jnp.concatenate([b[0], b[1], b[0]], axis=dims[0][1][0])
    return dot(lhs, rhs, dims)


def dot_left(a, b, dims=NN):
    lhs = jnp.concatenate([a[0], a[1]], axis=dims[0][0][0])
    rhs = jnp.concatenate([b, b], axis=dims[0][1][0])
    return dot(lhs, rhs, dims)


def dot_right(a, b, dims=NN):
    lhs = jnp.concatenate([a, a], axis=dims[0][0][0])
    rhs = jnp.concatenate([b[0], b[1]], axis=dims[0][1][0])
    return dot(lhs, rhs, dims)


def iota2(shape, axis):
    return lax.broadcasted_iota(jnp.int32, shape, axis)


def upper_ones(size):
    return (iota2((size, size), 0) <= iota2((size, size), 1)).astype(F32)


def fetch(sems, *pairs):
    copies = [pltpu.make_async_copy(src, dst, sems.at[i]) for i, (src, dst) in enumerate(pairs)]
    for copy in copies:
        copy.start()
    for copy in copies:
        copy.wait()


def pack_kernel(k_hbm, v_hbm, gate_hbm, out_ref, k_ref, v_ref, gate_ref, sems):
    fetch(sems, (k_hbm, k_ref), (v_hbm, v_ref), (gate_hbm, gate_ref))
    rows = k_ref.shape[0]
    heads = gate_ref.shape[0]
    out_ref[0:rows, :] = k_ref[...].astype(F32).T.astype(BF16)
    out_ref[rows : 2 * rows, :] = v_ref[...]
    gate = gate_ref[...]
    high = gate.astype(BF16).astype(F32)
    middle = (gate - high).astype(BF16).astype(F32)
    low = gate - high - middle
    blank = jnp.zeros((GATE_ROWS - 3 * heads, gate.shape[1]), F32)
    out_ref[2 * rows :, :] = jnp.concatenate([high, middle, low, blank], axis=0).astype(BF16)


def local_kernel(
    packed_ref, level_hbm, q_hbm, qmap_hbm, kmap_hbm, qp_ref, qt_ref, sd_ref, mix_ref, loc_ref,
    q_ref, qmap_ref, kmap_ref, level_ref, sems,
):
    fetch(sems, (q_hbm, q_ref), (qmap_hbm, qmap_ref), (kmap_hbm, kmap_ref), (level_hbm, level_ref))
    heads, dim, _ = qmap_ref.shape
    width, rows = packed_ref.shape
    low_bits = rows.bit_length() - 1
    piece = packed_ref[width - GATE_ROWS :, :].astype(F32)
    gate = piece[0:heads] + piece[heads : 2 * heads] + piece[2 * heads : 3 * heads]
    cum = exact_dot(gate, upper_ones(rows))
    cum_t = cum.T
    kt = packed_ref[0:rows, :]
    v = packed_ref[rows : 2 * rows, :]
    row, col = iota2((rows, rows), 0), iota2((rows, rows), 1)
    causal = col <= row
    differ = row ^ col
    highs, lows = [], []
    for h in range(heads):
        qp = dot_right(q_ref[:, h * dim : (h + 1) * dim], halves(qmap_ref[h]))
        qp_ref[h] = qp
        qt = dot_f32(halves(qp), halves(kmap_ref[h]), NT)
        qt_ref[h] = qt
        high, low = halves(qt)
        highs.append(high)
        lows.append(low)
    score = dot_left((jnp.concatenate(highs, axis=0), jnp.concatenate(lows, axis=0)), kt)
    highs, lows = [], []
    for h in range(heads):
        decay = jnp.exp(jnp.where(causal, cum_t[:, h : h + 1] - cum[h : h + 1, :], NEGATIVE))
        weight = jnp.full((rows, rows), level_ref[h, 0], F32)
        for level in range(1, low_bits + 1):
            weight = jnp.where(differ >= (1 << (level - 1)), level_ref[h, level], weight)
        decayed = score[h * rows : (h + 1) * rows] * decay
        mix_ref[h] = decay * weight
        sd_ref[h] = decayed
        high, low = halves(decayed * weight)
        highs.append(high)
        lows.append(low)
    loc = dot_left((jnp.concatenate(highs, axis=0), jnp.concatenate(lows, axis=0)), v)
    for h in range(heads):
        loc_ref[h] = loc[h * rows : (h + 1) * rows]


def stacked_queries(q_ref, dim):
    return jnp.concatenate([q_ref[:, at : at + dim] for at in range(0, q_ref.shape[1], dim)], axis=0)


def pair_decay(span, even_ref, odd_ref, heads):
    pairs, width, rows = even_ref.shape
    gates = []
    for ref in (even_ref, odd_ref):
        for p in range(pairs):
            piece = ref[p, width - GATE_ROWS :, :].astype(F32)
            gates.append(piece[0:heads] + piece[heads : 2 * heads] + piece[2 * heads : 3 * heads])
    cum = exact_dot(jnp.concatenate(gates, axis=0), upper_ones(rows))
    cum_e, cum_o = cum[: pairs * heads], cum[pairs * heads :]
    end_e = jnp.broadcast_to(cum_e[:, rows - 1 : rows], cum_e.shape)
    end_o = jnp.broadcast_to(cum_o[:, rows - 1 : rows], cum_o.shape)
    odd_span = (span & 1) == 1
    decay_e = jnp.exp(end_e - cum_e + jnp.where(odd_span, 0.0, end_o))
    decay_o = jnp.exp(end_o - cum_o + jnp.where(odd_span, end_e, 0.0))
    return cum_e, cum_o, end_e, end_o, decay_e, decay_o


def pair_blocks(even_ref, odd_ref, p, rows):
    kt = jnp.concatenate([even_ref[p, 0:rows, :], odd_ref[p, 0:rows, :]], axis=1)
    v = jnp.concatenate([even_ref[p, rows : 2 * rows, :], odd_ref[p, rows : 2 * rows, :]], axis=0)
    return kt, v


def pair_state(kt, v, weight, state_ref, p):
    heads = weight.shape[0]
    dim = kt.shape[0]
    kt32 = kt.astype(F32)
    highs, lows = [], []
    for h in range(heads):
        high, low = halves(kt32 * weight[h : h + 1, :])
        highs.append(high)
        lows.append(low)
    state = dot_left((jnp.concatenate(highs, axis=0), jnp.concatenate(lows, axis=0)), v)
    for h in range(heads):
        state_ref[p, h] = state[h * dim : (h + 1) * dim]


def early_kernel(
    span_ref, q_ref, even_ref, odd_ref, score_ref, peak_ref, state_ref, ends_ref, before_ref, decay_scr, *, offsets,
):
    pairs, heads, dim, _ = state_ref.shape
    rows = even_ref.shape[2]
    span = span_ref[0]
    _, cum_o, end_e, end_o, decay_e, decay_o = pair_decay(span, even_ref, odd_ref, heads)
    ends_ref[...] = end_e + end_o
    before_ref[...] = end_o[0:heads]
    for p in range(pairs):
        at = slice(p * heads, (p + 1) * heads)
        if p == 0:
            first = jnp.concatenate([jnp.zeros_like(decay_e[at]), jnp.exp(end_o[at] - cum_o[at])], axis=1)
            decay_scr[p] = first
        else:
            decay_scr[p] = jnp.concatenate([decay_e[at], decay_o[at]], axis=1)
    q_all = stacked_queries(q_ref, dim)
    scale = dim ** (-0.5)
    row, col = iota2((rows, 2 * rows), 0), iota2((rows, 2 * rows), 1)
    odd_span = (span & 1) == 1
    seen = (col <= row) | ((col >= rows) & odd_span)
    kt, v = pair_blocks(even_ref, odd_ref, 0, rows)
    score = dot(q_all, kt) * scale
    score = jnp.where(jnp.concatenate([seen] * heads, axis=0), score, NEGATIVE)
    score_ref[0] = score
    peak_ref[...] = jnp.maximum(score[:, :rows], score[:, rows:])

    @pl.when(odd_span)
    def _():
        pair_state(kt, v, decay_scr[0], state_ref, 0)

    for p in range(1, pairs):

        @pl.when((span ^ offsets[p]) < span)
        def _(p=p):
            kt, v = pair_blocks(even_ref, odd_ref, p, rows)
            score = dot(q_all, kt) * scale
            score_ref[p] = score
            peak_ref[...] = jnp.maximum(peak_ref[...], jnp.maximum(score[:, :rows], score[:, rows:]))
            pair_state(kt, v, decay_scr[p], state_ref, p)


def forward_kernel(
    span_ref, level_ref, q_ref, even_a_ref, odd_a_ref, even_b_ref, odd_b_ref, score_a_ref, peak_a_ref, state_a_ref,
    ends_a_ref, before_ref, qt_ref, loc_ref, gain_ref, gate_ref,
    raw_ref, target_ref, level_state_ref, comb_ref, sums_ref,
    score_scr, peak_scr, state_scr, total_scr, acc_scr, *, offsets,
):
    heads, rows, dim = qt_ref.shape
    early, late = even_a_ref.shape[0], even_b_ref.shape[0]
    pairs = early + late
    span_bits = level_state_ref.shape[0]
    low_bits = rows.bit_length() - 1
    span = span_ref[0]
    odd_span = (span & 1) == 1
    scale = dim ** (-0.5)
    q_all = stacked_queries(q_ref, dim)
    _, _, end_e, end_o, decay_e, decay_o = pair_decay(span, even_b_ref, odd_b_ref, heads)
    peak_scr[...] = peak_a_ref[...]
    for p in range(late):

        @pl.when((span ^ offsets[early + p]) < span)
        def _(p=p):
            at = slice(p * heads, (p + 1) * heads)
            kt, v = pair_blocks(even_b_ref, odd_b_ref, p, rows)
            score = dot(q_all, kt) * scale
            score_scr[p] = score
            peak_scr[...] = jnp.maximum(peak_scr[...], jnp.maximum(score[:, :rows], score[:, rows:]))
            pair_state(kt, v, jnp.concatenate([decay_e[at], decay_o[at]], axis=1), state_scr, p)

    ends = jnp.concatenate([ends_a_ref[...], end_e + end_o], axis=0)
    size = pairs * heads

    def pair_of(index):
        position = index // heads
        offset = position * 0
        for p in range(pairs):
            offset = jnp.where(position == p, offsets[p], offset)
        return (span ^ offset) >> 1, index % heads

    mine, my_head = pair_of(iota2((size, size), 0))
    other, other_head = pair_of(iota2((size, size), 1))
    between = (other > mine) & (other < (span >> 1)) & (my_head == other_head)
    carried = exact_dot(between.astype(F32), ends)
    before = jnp.where(odd_span, before_ref[...], 0.0)
    factor = jnp.exp(carried + jnp.concatenate([before] * pairs, axis=0))

    peak = jnp.max(peak_scr[...], axis=1, keepdims=True)
    peak_scr[...] = jnp.broadcast_to(peak, peak_scr.shape)

    def weigh(score, v):
        top = peak_scr[...]
        left = jnp.exp(score[:, :rows] - top)
        right = jnp.exp(score[:, rows:] - top)
        total = left + right
        return total, dot(jnp.concatenate([left.astype(BF16), right.astype(BF16)], axis=1), v)

    total_scr[...], acc_scr[...] = weigh(score_a_ref[0], pair_blocks(even_a_ref, odd_a_ref, 0, rows)[1])
    for p in range(1, pairs):

        @pl.when((span ^ offsets[p]) < span)
        def _(p=p):
            if p < early:
                total, acc = weigh(score_a_ref[p], pair_blocks(even_a_ref, odd_a_ref, p, rows)[1])
            else:
                q = p - early
                total, acc = weigh(score_scr[q], pair_blocks(even_b_ref, odd_b_ref, q, rows)[1])
            total_scr[...] += total
            acc_scr[...] += acc

    for level in range(span_bits):
        members = [p for p in range(pairs) if max(offsets[p], 1).bit_length() - 1 == level]
        used = ((span >> level) & 1) == 1

        @pl.when(used)
        def _(members=members, level=level):
            for h in range(heads):
                value = None
                for p in members:
                    state = state_a_ref[p, h] if p < early else state_scr[p - early, h]
                    if p > 0:
                        state = state * factor[p * heads + h : p * heads + h + 1, :]
                    value = state if value is None else value + state
                level_state_ref[level, h] = value

        @pl.when(jnp.logical_not(used))
        def _(level=level):
            level_state_ref[level] = jnp.zeros_like(level_state_ref[level])

    total = jnp.sum(total_scr[...], axis=1, keepdims=True)
    target_all = acc_scr[...] / total
    entry = jnp.exp(exact_dot(gate_ref[...], upper_ones(rows)).T)
    squares = jnp.zeros((rows, dim), F32)
    gained = jnp.zeros((rows, dim), F32)
    crossed = jnp.zeros((rows, dim), F32)
    for h in range(heads):
        combined = jnp.zeros((dim, dim), F32)
        for level in range(span_bits):
            combined = combined + level_ref[h, low_bits + 1 + level] * level_state_ref[level, h]
        comb_ref[h] = combined
        far = entry[:, h : h + 1] * dot_f32(halves(qt_ref[h]), halves(combined))
        raw = loc_ref[h] + far
        target = target_all[h * rows : (h + 1) * rows]
        raw_ref[h] = raw
        target_ref[h] = target
        gain = gain_ref[h : h + 1, :]
        square = raw * raw
        squares = squares + square
        gained = gained + square * (gain * gain)
        crossed = crossed + target * raw * gain
    lanes = iota2((rows, rows), 1)
    columns = jnp.where(
        lanes == 0,
        jnp.sum(squares, axis=1, keepdims=True),
        jnp.where(
            lanes == 1,
            jnp.sum(gained, axis=1, keepdims=True),
            jnp.where(lanes == 2, jnp.sum(crossed, axis=1, keepdims=True), 0.0),
        ),
    )
    sums_ref[...] = columns.T[0:8]


def chunk_of(head, heads, span, splits):
    group = heads >> len(splits)
    chunk = 0
    for place, stride in enumerate(splits):
        shift = len(splits) - 1 - place
        bit = (head // group >> shift) & 1
        chunk = chunk + ((bit ^ ((span // stride) & 1)) << shift)
    return chunk * group + head % group


def backward_kernel(
    span_ref, sums_a_ref, sums_b_ref, gate_ref, q_ref, k_ref, v_ref, kmap_ref, gain_ref,
    qp_ref, qt_ref, sd_ref, mix_ref, raw_ref, target_ref, state_ref, comb_ref,
    keep_ref, send_ref, *, norm_width, total_tokens, splits, heads,
):
    _, rows, dim = qt_ref.shape
    share = len(heads)
    span_bits = state_ref.shape[0]
    low_bits = rows.bit_length() - 1
    span = span_ref[0]
    first = (span & 1) == 0
    sums = (sums_a_ref[...] + sums_b_ref[...]).T
    squares, gained, crossed = sums[:, 0:1], sums[:, 1:2], sums[:, 2:3]
    inverse = lax.rsqrt(squares / norm_width + EPSILON)
    inner = (inverse * gained - crossed) / total_tokens
    shrink = inverse * inverse * inverse * inner / norm_width
    entry = jnp.exp(exact_dot(gate_ref[...], upper_ones(rows)).T)
    k = k_ref[...]
    v = v_ref[...]
    row, col = iota2((rows, rows), 0), iota2((rows, rows), 1)
    differ = row ^ col
    levels = low_bits + 1 + span_bits
    pad = 16
    gain_rows, residuals, highs, lows = [], [], [], []
    for h in heads:
        gain = gain_ref[h : h + 1, :]
        raw = raw_ref[h]
        normed = raw * inverse
        mismatch = (normed * gain - target_ref[h]) / total_tokens
        gain_rows.append(jnp.sum(mismatch * normed, axis=0, keepdims=True))
        residual = inverse * (mismatch * gain) - raw * shrink
        residuals.append(residual)
        high, low = halves(residual)
        highs.append(high)
        lows.append(low)
    d_mix = dot_left((jnp.concatenate(highs, axis=0), jnp.concatenate(lows, axis=0)), v, NT)
    level_rows, highs, lows = [], [], []
    for i, h in enumerate(heads):
        d_mix_h = d_mix[i * rows : (i + 1) * rows]
        high, low = halves(d_mix_h * mix_ref[h])
        highs.append(high)
        lows.append(low)
        through = d_mix_h * sd_ref[h]
        mine = []
        for level in range(low_bits + 1):
            least = 0 if level == 0 else 1 << (level - 1)
            here = (differ >= least) & (differ < (1 << level))
            mine.append(jnp.sum(jnp.where(here, through, 0.0), axis=0, keepdims=True))
        level_rows.append(mine)
    d_local = dot_left((jnp.concatenate(highs, axis=0), jnp.concatenate(lows, axis=0)), k)
    for i, h in enumerate(heads):
        lead = halves(entry[:, h : h + 1] * residuals[i])
        d_qt = halves(d_local[i * rows : (i + 1) * rows] + dot_f32(lead, halves(comb_ref[h]), NT))
        grad_k = dot_f32(d_qt, halves(qp_ref[h]), TN)
        d_qp = dot_f32(d_qt, halves(kmap_ref[h]))
        grad_q = dot_right(q_ref[:, h * dim : (h + 1) * dim], halves(d_qp), TN)
        d_comb = dot_f32(halves(qt_ref[h]), lead, TN)
        for level in range(span_bits):
            level_rows[i].append(jnp.sum(state_ref[level, h] * d_comb, axis=0, keepdims=True))
        level_rows[i].append(jnp.zeros((pad - levels, rows), F32))
        at = pl.ds(pl.multiple_of(chunk_of(i, share, span, splits) * dim, dim), dim)
        keep_ref[at, :] = jnp.where(first, grad_q, grad_k)
        send_ref[at, :] = jnp.where(first, grad_k, grad_q)
    table = jnp.sum(jnp.concatenate([r for mine in level_rows for r in mine], axis=0), axis=1, keepdims=True)
    spread = iota2((share * pad, rows), 0) % pad == iota2((share * pad, rows), 1)
    pick = iota2((share, share * pad), 1) // pad == iota2((share, share * pad), 0)
    level_sums = exact_dot(pick.astype(F32), jnp.where(spread, table, 0.0))
    small = jnp.concatenate(gain_rows + [level_sums], axis=0)
    tail = pl.ds(share * dim, 2 * share)
    keep_ref[tail, :] = small
    send_ref[tail, :] = small


def place_kernel(span_ref, *refs, splits):
    q_ref, k_ref = refs[-2:]
    heads, dim, _ = q_ref.shape
    parts = (len(refs) - 2) // 2
    share = heads // parts
    span = span_ref[0]
    first = (span & 1) == 0
    for h in range(heads):
        mine_ref, other_ref = refs[2 * (h // share) : 2 * (h // share) + 2]
        at = pl.ds(pl.multiple_of(chunk_of(h % share, share, span, splits) * dim, dim), dim)
        mine, other = mine_ref[at, :], other_ref[at, :]
        q_ref[h] = jnp.where(first, mine, other)
        k_ref[h] = jnp.where(first, other, mine)


def vmem(count):
    return [pl.BlockSpec(memory_space=pltpu.VMEM)] * count


def hbm(count):
    return [pl.BlockSpec(memory_space=pltpu.HBM)] * count


def smem(count):
    return [pl.BlockSpec(memory_space=pltpu.SMEM)] * count


def shape(*dims, dtype=F32):
    return jax.ShapeDtypeStruct(dims, dtype)


def call(kernel, ins, outs, limit, flops, scratch=(), **static):
    body = functools.partial(kernel, **static) if static else kernel
    single = not isinstance(outs, (list, tuple))
    return pl.pallas_call(
        body,
        out_shape=outs,
        in_specs=ins,
        out_specs=pl.BlockSpec(memory_space=pltpu.VMEM) if single else vmem(len(outs)),
        scratch_shapes=list(scratch),
        compiler_params=pltpu.CompilerParams(vmem_limit_bytes=limit << 20),
        cost_estimate=pl.CostEstimate(flops=flops, bytes_accessed=1 << 20, transcendentals=0),
    )


def in_hbm(*values):
    return [pltpu.with_memory_space_constraint(value, pltpu.HBM) for value in values]


def swap(value, axis, stride):
    count = lax.axis_size(axis)
    return lax.ppermute(value, axis, [(i, i ^ stride) for i in range(count)])


def on_device(queries, key_vectors, value_vectors, log_gate, query_map, key_map, level_weight, norm_gain):
    rows, dim = key_vectors.shape
    heads = queries.shape[1] // dim
    count = lax.axis_size("seq")
    groups = lax.axis_size("head")
    span_bits = count.bit_length() - 1
    span = lax.axis_index("seq").astype(jnp.int32).reshape(1)
    total_tokens = rows * count
    norm_width = heads * dim * groups
    gain = norm_gain.reshape(heads, dim)
    strides = [1 << bit for bit in reversed(range(1, span_bits))]
    splits = (2, 4)
    cube = (heads, dim, dim)
    packed_rows = 2 * rows + GATE_ROWS

    offsets = [0]
    for stride in strides:
        offsets += [offset + stride for offset in offsets]
    early = len(offsets) // 2

    packed = call(pack_kernel, hbm(3), shape(packed_rows, rows, dtype=BF16), 8, 1 << 20, scratch=[
        pltpu.VMEM((rows, dim), BF16),
        pltpu.VMEM((rows, dim), BF16),
        pltpu.VMEM((heads, rows), F32),
        pltpu.SemaphoreType.DMA((3,)),
    ])(*in_hbm(key_vectors, value_vectors, log_gate))
    qp, qt, score_decay, mix, local = call(
        local_kernel, vmem(1) + hbm(4), [shape(*cube)] * 5, 24, 1 << 29,
        scratch=[
            pltpu.VMEM(queries.shape, BF16),
            pltpu.VMEM(cube, F32),
            pltpu.VMEM(cube, F32),
            pltpu.SMEM(level_weight.shape, F32),
            pltpu.SemaphoreType.DMA((4,)),
        ],
    )(packed, *in_hbm(level_weight, queries, query_map, key_map))

    even_a = packed[None]
    for stride in strides[:-1]:
        received = swap(even_a, "seq", stride)
        even_a = jnp.concatenate([even_a, received], axis=0)
    even_b = swap(even_a, "seq", strides[-1])
    odd_a = swap(even_a, "seq", 1)
    odd_b = swap(even_b, "seq", 1)

    scores, peaks, states, ends, before = call(
        early_kernel,
        smem(1) + vmem(3),
        [
            shape(early, heads * rows, 2 * rows),
            shape(heads * rows, rows),
            shape(early, *cube),
            shape(early * heads, rows),
            shape(heads, rows),
        ],
        24,
        1 << 30,
        scratch=[pltpu.VMEM((early, heads, 2 * rows), F32)],
        offsets=tuple(offsets),
    )(span, queries, even_a, odd_a)
    raw, target, level_states, combined, sums = call(
        forward_kernel,
        smem(2) + vmem(14),
        [shape(*cube), shape(*cube), shape(span_bits, *cube), shape(*cube), shape(8, rows)],
        32,
        1 << 31,
        scratch=[
            pltpu.VMEM((early, heads * rows, 2 * rows), F32),
            pltpu.VMEM((heads * rows, rows), F32),
            pltpu.VMEM((early, *cube), F32),
            pltpu.VMEM((heads * rows, rows), F32),
            pltpu.VMEM((heads * rows, dim), F32),
        ],
        offsets=tuple(offsets),
    )(
        span, level_weight, queries, even_a, odd_a, even_b, odd_b, scores, peaks, states, ends, before,
        qt, local, gain, log_gate,
    )

    stride = 1
    while stride < groups:
        received = swap(sums, "head", stride)
        if 2 * stride < groups:
            sums = sums + received
        stride *= 2

    share = heads // PARTS
    size = share * dim
    held = []
    for part in range(PARTS):
        keep, send = call(
            backward_kernel,
            smem(1) + vmem(16),
            [shape(share * (dim + 2), dim)] * 2,
            24,
            1 << 29,
            norm_width=float(norm_width),
            total_tokens=float(total_tokens),
            splits=splits,
            heads=range(part * share, (part + 1) * share),
        )(
            span, sums, received, log_gate, queries, key_vectors, value_vectors, key_map, gain,
            qp, qt, score_decay, mix, raw, target, level_states, combined,
        )
        held.append(keep + swap(send, "seq", 1))
    for split in splits:
        size //= 2
        for part in range(PARTS):
            here = held[part]
            got = swap(here[size:], "seq", split)
            held[part] = jnp.concatenate([here[:size] + got[:size], here[2 * size :] + got[size:]])
    for stride in strides:
        if stride not in splits:
            for part in range(PARTS):
                held[part] = held[part] + swap(held[part], "seq", stride)
    small = [here[size:] for here in held]
    mine = [here[:size] for here in held]
    for split in reversed(splits):
        for part in range(PARTS):
            mine[part] = jnp.concatenate([mine[part], swap(mine[part], "seq", split)])
    pieces = []
    for part in range(PARTS):
        pieces += [mine[part], swap(mine[part], "seq", 1)]
    grad_query, grad_key = call(
        place_kernel, smem(1) + vmem(2 * PARTS), [shape(*cube)] * 2, 16, 1 << 20, splits=splits
    )(span, *pieces)
    grad_gain = jnp.concatenate([piece[:share] for piece in small]).reshape(-1)
    grad_levels = jnp.concatenate([piece[share:, : level_weight.shape[1]] for piece in small])
    return grad_query, grad_key, grad_levels, grad_gain


def solution(mesh):
    placed = (
        P("seq", "head"),
        P("seq", "head"),
        P("seq", "head"),
        P("head", "seq"),
        P("head", None, None),
        P("head", None, None),
        P("head", None),
        P("head"),
    )

    return jax.shard_map(
        on_device,
        mesh=mesh,
        in_specs=placed,
        out_specs=(P("head", None, None), P("head", None, None), P("head", None), P("head")),
        check_vma=False,
    )
```

```python
import functools

import jax
import jax.numpy as jnp
from jax import lax
from jax.experimental import pallas as pl
from jax.experimental.pallas import tpu as pltpu
from jax.sharding import PartitionSpec as P


HIGHEST = lax.Precision.HIGHEST
NEGATIVE = -1e30
EPSILON = 1e-05
F32 = jnp.float32
BF16 = jnp.bfloat16
NN = (((1,), (0,)), ((), ()))
NT = (((1,), (1,)), ((), ()))
TN = (((0,), (0,)), ((), ()))
GATE_ROWS = 32
PARTS = 2


def dot(a, b, dims=NN):
    return lax.dot_general(a, b, dims, preferred_element_type=F32)


def exact_dot(a, b, dims=NN):
    return lax.dot_general(a, b, dims, precision=HIGHEST, preferred_element_type=F32)


def halves(x):
    high = x.astype(BF16)
    return high, (x - high.astype(F32)).astype(BF16)


def dot_f32(a, b, dims=NN):
    lhs = jnp.concatenate([a[0], a[0], a[1]], axis=dims[0][0][0])
    rhs = jnp.concatenate([b[0], b[1], b[0]], axis=dims[0][1][0])
    return dot(lhs, rhs, dims)


def dot_left(a, b, dims=NN):
    lhs = jnp.concatenate([a[0], a[1]], axis=dims[0][0][0])
    rhs = jnp.concatenate([b, b], axis=dims[0][1][0])
    return dot(lhs, rhs, dims)


def dot_right(a, b, dims=NN):
    lhs = jnp.concatenate([a, a], axis=dims[0][0][0])
    rhs = jnp.concatenate([b[0], b[1]], axis=dims[0][1][0])
    return dot(lhs, rhs, dims)


def iota2(shape, axis):
    return lax.broadcasted_iota(jnp.int32, shape, axis)


def upper_ones(size):
    return (iota2((size, size), 0) <= iota2((size, size), 1)).astype(F32)


def fetch(sems, *pairs):
    copies = [pltpu.make_async_copy(src, dst, sems.at[i]) for i, (src, dst) in enumerate(pairs)]
    for copy in copies:
        copy.start()
    for copy in copies:
        copy.wait()


def pack_kernel(k_hbm, v_hbm, gate_hbm, out_ref, k_ref, v_ref, gate_ref, sems):
    fetch(sems, (k_hbm, k_ref), (v_hbm, v_ref), (gate_hbm, gate_ref))
    rows = k_ref.shape[0]
    heads = gate_ref.shape[0]
    out_ref[0:rows, :] = k_ref[...].astype(F32).T.astype(BF16)
    out_ref[rows : 2 * rows, :] = v_ref[...]
    gate = gate_ref[...]
    high = gate.astype(BF16).astype(F32)
    middle = (gate - high).astype(BF16).astype(F32)
    low = gate - high - middle
    blank = jnp.zeros((GATE_ROWS - 3 * heads, gate.shape[1]), F32)
    out_ref[2 * rows :, :] = jnp.concatenate([high, middle, low, blank], axis=0).astype(BF16)


def local_kernel(
    packed_ref, level_hbm, q_hbm, qmap_hbm, kmap_hbm, qp_ref, qt_ref, sd_ref, mix_ref, loc_ref,
    q_ref, qmap_ref, kmap_ref, level_ref, sems,
):
    fetch(sems, (q_hbm, q_ref), (qmap_hbm, qmap_ref), (kmap_hbm, kmap_ref), (level_hbm, level_ref))
    heads, dim, _ = qmap_ref.shape
    width, rows = packed_ref.shape
    low_bits = rows.bit_length() - 1
    piece = packed_ref[width - GATE_ROWS :, :].astype(F32)
    gate = piece[0:heads] + piece[heads : 2 * heads] + piece[2 * heads : 3 * heads]
    cum = exact_dot(gate, upper_ones(rows))
    cum_t = cum.T
    kt = packed_ref[0:rows, :]
    v = packed_ref[rows : 2 * rows, :]
    row, col = iota2((rows, rows), 0), iota2((rows, rows), 1)
    causal = col <= row
    differ = row ^ col
    highs, lows = [], []
    for h in range(heads):
        qp = dot_right(q_ref[:, h * dim : (h + 1) * dim], halves(qmap_ref[h]))
        qp_ref[h] = qp
        qt = dot_f32(halves(qp), halves(kmap_ref[h]), NT)
        qt_ref[h] = qt
        high, low = halves(qt)
        highs.append(high)
        lows.append(low)
    score = dot_left((jnp.concatenate(highs, axis=0), jnp.concatenate(lows, axis=0)), kt)
    highs, lows = [], []
    for h in range(heads):
        decay = jnp.exp(jnp.where(causal, cum_t[:, h : h + 1] - cum[h : h + 1, :], NEGATIVE))
        weight = jnp.full((rows, rows), level_ref[h, 0], F32)
        for level in range(1, low_bits + 1):
            weight = jnp.where(differ >= (1 << (level - 1)), level_ref[h, level], weight)
        decayed = score[h * rows : (h + 1) * rows] * decay
        mix_ref[h] = decay * weight
        sd_ref[h] = decayed
        high, low = halves(decayed * weight)
        highs.append(high)
        lows.append(low)
    loc = dot_left((jnp.concatenate(highs, axis=0), jnp.concatenate(lows, axis=0)), v)
    for h in range(heads):
        loc_ref[h] = loc[h * rows : (h + 1) * rows]


def stacked_queries(q_ref, dim):
    return jnp.concatenate([q_ref[:, at : at + dim] for at in range(0, q_ref.shape[1], dim)], axis=0)


def pair_decay(span, even_ref, odd_ref, heads):
    pairs, width, rows = even_ref.shape
    gates = []
    for ref in (even_ref, odd_ref):
        for p in range(pairs):
            piece = ref[p, width - GATE_ROWS :, :].astype(F32)
            gates.append(piece[0:heads] + piece[heads : 2 * heads] + piece[2 * heads : 3 * heads])
    cum = exact_dot(jnp.concatenate(gates, axis=0), upper_ones(rows))
    cum_e, cum_o = cum[: pairs * heads], cum[pairs * heads :]
    end_e = jnp.broadcast_to(cum_e[:, rows - 1 : rows], cum_e.shape)
    end_o = jnp.broadcast_to(cum_o[:, rows - 1 : rows], cum_o.shape)
    odd_span = (span & 1) == 1
    decay_e = jnp.exp(end_e - cum_e + jnp.where(odd_span, 0.0, end_o))
    decay_o = jnp.exp(end_o - cum_o + jnp.where(odd_span, end_e, 0.0))
    return cum_e, cum_o, end_e, end_o, decay_e, decay_o


def pair_blocks(even_ref, odd_ref, p, rows):
    kt = jnp.concatenate([even_ref[p, 0:rows, :], odd_ref[p, 0:rows, :]], axis=1)
    v = jnp.concatenate([even_ref[p, rows : 2 * rows, :], odd_ref[p, rows : 2 * rows, :]], axis=0)
    return kt, v


def pair_state(kt, v, weight, state_ref, p):
    heads = weight.shape[0]
    dim = kt.shape[0]
    kt32 = kt.astype(F32)
    highs, lows = [], []
    for h in range(heads):
        high, low = halves(kt32 * weight[h : h + 1, :])
        highs.append(high)
        lows.append(low)
    state = dot_left((jnp.concatenate(highs, axis=0), jnp.concatenate(lows, axis=0)), v)
    for h in range(heads):
        state_ref[p, h] = state[h * dim : (h + 1) * dim]


def by_level(offsets):
    levels = {}
    for p, offset in enumerate(offsets):
        if p > 0:
            levels.setdefault(offset.bit_length() - 1, []).append(p)
    return sorted(levels.items())


def early_kernel(
    span_ref, q_ref, even_ref, odd_ref, score_ref, peak_ref, state_ref, ends_ref, before_ref, decay_scr, *, offsets,
):
    pairs, heads, dim, _ = state_ref.shape
    rows = even_ref.shape[2]
    span = span_ref[0]
    _, cum_o, end_e, end_o, decay_e, decay_o = pair_decay(span, even_ref, odd_ref, heads)
    ends_ref[...] = end_e + end_o
    before_ref[...] = end_o[0:heads]
    for p in range(pairs):
        at = slice(p * heads, (p + 1) * heads)
        if p == 0:
            first = jnp.concatenate([jnp.zeros_like(decay_e[at]), jnp.exp(end_o[at] - cum_o[at])], axis=1)
            decay_scr[p] = first
        else:
            decay_scr[p] = jnp.concatenate([decay_e[at], decay_o[at]], axis=1)
    q_all = stacked_queries(q_ref, dim)
    scale = dim ** (-0.5)
    row, col = iota2((rows, 2 * rows), 0), iota2((rows, 2 * rows), 1)
    odd_span = (span & 1) == 1
    seen = (col <= row) | ((col >= rows) & odd_span)
    kt, v = pair_blocks(even_ref, odd_ref, 0, rows)
    score = dot(q_all, kt) * scale
    score = jnp.where(jnp.concatenate([seen] * heads, axis=0), score, NEGATIVE)
    score_ref[0] = score
    peak_ref[...] = jnp.maximum(score[:, :rows], score[:, rows:])

    @pl.when(odd_span)
    def _():
        pair_state(kt, v, decay_scr[0], state_ref, 0)

    for bit, members in by_level(offsets[:pairs]):

        @pl.when(((span >> bit) & 1) == 1)
        def _(members=members):
            top = peak_ref[...]
            blocks = [pair_blocks(even_ref, odd_ref, p, rows) for p in members]
            for p, (kt, _) in zip(members, blocks):
                score = dot(q_all, kt) * scale
                score_ref[p] = score
                top = jnp.maximum(top, jnp.maximum(score[:, :rows], score[:, rows:]))
            peak_ref[...] = top
            for p, (kt, v) in zip(members, blocks):
                pair_state(kt, v, decay_scr[p], state_ref, p)


def forward_kernel(
    span_ref, level_ref, q_ref, even_a_ref, odd_a_ref, even_b_ref, odd_b_ref, score_a_ref, peak_a_ref, state_a_ref,
    ends_a_ref, before_ref, qt_ref, loc_ref, gain_ref, gate_ref,
    raw_ref, target_ref, level_state_ref, comb_ref, sums_ref,
    score_scr, peak_scr, state_scr, total_scr, acc_scr, *, offsets,
):
    heads, rows, dim = qt_ref.shape
    early, late = even_a_ref.shape[0], even_b_ref.shape[0]
    pairs = early + late
    span_bits = level_state_ref.shape[0]
    low_bits = rows.bit_length() - 1
    span = span_ref[0]
    odd_span = (span & 1) == 1
    scale = dim ** (-0.5)
    q_all = stacked_queries(q_ref, dim)
    _, _, end_e, end_o, decay_e, decay_o = pair_decay(span, even_b_ref, odd_b_ref, heads)
    peak_scr[...] = peak_a_ref[...]
    for bit, members in by_level(offsets):
        members = [p - early for p in members if p >= early]
        if not members:
            continue

        @pl.when(((span >> bit) & 1) == 1)
        def _(members=members):
            top = peak_scr[...]
            blocks = [pair_blocks(even_b_ref, odd_b_ref, p, rows) for p in members]
            for p, (kt, _) in zip(members, blocks):
                score = dot(q_all, kt) * scale
                score_scr[p] = score
                top = jnp.maximum(top, jnp.maximum(score[:, :rows], score[:, rows:]))
            peak_scr[...] = top
            for p, (kt, v) in zip(members, blocks):
                at = slice(p * heads, (p + 1) * heads)
                pair_state(kt, v, jnp.concatenate([decay_e[at], decay_o[at]], axis=1), state_scr, p)

    ends = jnp.concatenate([ends_a_ref[...], end_e + end_o], axis=0)
    size = pairs * heads

    def pair_of(index):
        position = index // heads
        offset = position * 0
        for p in range(pairs):
            offset = jnp.where(position == p, offsets[p], offset)
        return (span ^ offset) >> 1, index % heads

    mine, my_head = pair_of(iota2((size, size), 0))
    other, other_head = pair_of(iota2((size, size), 1))
    between = (other > mine) & (other < (span >> 1)) & (my_head == other_head)
    carried = exact_dot(between.astype(F32), ends)
    before = jnp.where(odd_span, before_ref[...], 0.0)
    factor = jnp.exp(carried + jnp.concatenate([before] * pairs, axis=0))

    peak = jnp.max(peak_scr[...], axis=1, keepdims=True)
    peak_scr[...] = jnp.broadcast_to(peak, peak_scr.shape)

    def weigh(members):
        top = peak_scr[...]
        total, weights, values = None, [], []
        for p in members:
            if p < early:
                score, v = score_a_ref[p], pair_blocks(even_a_ref, odd_a_ref, p, rows)[1]
            else:
                score, v = score_scr[p - early], pair_blocks(even_b_ref, odd_b_ref, p - early, rows)[1]
            left = jnp.exp(score[:, :rows] - top)
            right = jnp.exp(score[:, rows:] - top)
            total = left + right if total is None else total + (left + right)
            weights += [left.astype(BF16), right.astype(BF16)]
            values.append(v)
        return total, dot(jnp.concatenate(weights, axis=1), jnp.concatenate(values, axis=0))

    total_scr[...], acc_scr[...] = weigh([0])
    for bit, members in by_level(offsets):

        @pl.when(((span >> bit) & 1) == 1)
        def _(members=members):
            total, acc = weigh(members)
            total_scr[...] += total
            acc_scr[...] += acc

    for level in range(span_bits):
        members = [p for p in range(pairs) if max(offsets[p], 1).bit_length() - 1 == level]
        used = ((span >> level) & 1) == 1

        @pl.when(used)
        def _(members=members, level=level):
            for h in range(heads):
                value = None
                for p in members:
                    state = state_a_ref[p, h] if p < early else state_scr[p - early, h]
                    if p > 0:
                        state = state * factor[p * heads + h : p * heads + h + 1, :]
                    value = state if value is None else value + state
                level_state_ref[level, h] = value

        @pl.when(jnp.logical_not(used))
        def _(level=level):
            level_state_ref[level] = jnp.zeros_like(level_state_ref[level])

    total = jnp.sum(total_scr[...], axis=1, keepdims=True)
    target_all = acc_scr[...] / total
    entry = jnp.exp(exact_dot(gate_ref[...], upper_ones(rows)).T)
    squares = jnp.zeros((rows, dim), F32)
    gained = jnp.zeros((rows, dim), F32)
    crossed = jnp.zeros((rows, dim), F32)
    for h in range(heads):
        combined = jnp.zeros((dim, dim), F32)
        for level in range(span_bits):
            combined = combined + level_ref[h, low_bits + 1 + level] * level_state_ref[level, h]
        comb_ref[h] = combined
        far = entry[:, h : h + 1] * dot_f32(halves(qt_ref[h]), halves(combined))
        raw = loc_ref[h] + far
        target = target_all[h * rows : (h + 1) * rows]
        raw_ref[h] = raw
        target_ref[h] = target
        gain = gain_ref[h : h + 1, :]
        square = raw * raw
        squares = squares + square
        gained = gained + square * (gain * gain)
        crossed = crossed + target * raw * gain
    lanes = iota2((rows, rows), 1)
    columns = jnp.where(
        lanes == 0,
        jnp.sum(squares, axis=1, keepdims=True),
        jnp.where(
            lanes == 1,
            jnp.sum(gained, axis=1, keepdims=True),
            jnp.where(lanes == 2, jnp.sum(crossed, axis=1, keepdims=True), 0.0),
        ),
    )
    sums_ref[...] = columns.T[0:8]


def chunk_of(head, heads, span, splits):
    group = heads >> len(splits)
    chunk = 0
    for place, stride in enumerate(splits):
        shift = len(splits) - 1 - place
        bit = (head // group >> shift) & 1
        chunk = chunk + ((bit ^ ((span // stride) & 1)) << shift)
    return chunk * group + head % group


def backward_kernel(
    span_ref, sums_a_ref, sums_b_ref, gate_ref, q_ref, k_ref, v_ref, kmap_ref, gain_ref,
    qp_ref, qt_ref, sd_ref, mix_ref, raw_ref, target_ref, state_ref, comb_ref,
    keep_ref, send_ref, *, norm_width, total_tokens, splits, heads,
):
    _, rows, dim = qt_ref.shape
    share = len(heads)
    span_bits = state_ref.shape[0]
    low_bits = rows.bit_length() - 1
    span = span_ref[0]
    first = (span & 1) == 0
    sums = (sums_a_ref[...] + sums_b_ref[...]).T
    squares, gained, crossed = sums[:, 0:1], sums[:, 1:2], sums[:, 2:3]
    inverse = lax.rsqrt(squares / norm_width + EPSILON)
    inner = (inverse * gained - crossed) / total_tokens
    shrink = inverse * inverse * inverse * inner / norm_width
    entry = jnp.exp(exact_dot(gate_ref[...], upper_ones(rows)).T)
    k = k_ref[...]
    v = v_ref[...]
    row, col = iota2((rows, rows), 0), iota2((rows, rows), 1)
    differ = row ^ col
    levels = low_bits + 1 + span_bits
    pad = 16
    gain_rows, residuals, highs, lows = [], [], [], []
    for h in heads:
        gain = gain_ref[h : h + 1, :]
        raw = raw_ref[h]
        normed = raw * inverse
        mismatch = (normed * gain - target_ref[h]) / total_tokens
        gain_rows.append(jnp.sum(mismatch * normed, axis=0, keepdims=True))
        residual = inverse * (mismatch * gain) - raw * shrink
        residuals.append(residual)
        high, low = halves(residual)
        highs.append(high)
        lows.append(low)
    d_mix = dot_left((jnp.concatenate(highs, axis=0), jnp.concatenate(lows, axis=0)), v, NT)
    level_rows, highs, lows = [], [], []
    for i, h in enumerate(heads):
        d_mix_h = d_mix[i * rows : (i + 1) * rows]
        high, low = halves(d_mix_h * mix_ref[h])
        highs.append(high)
        lows.append(low)
        through = d_mix_h * sd_ref[h]
        mine = []
        for level in range(low_bits + 1):
            least = 0 if level == 0 else 1 << (level - 1)
            here = (differ >= least) & (differ < (1 << level))
            mine.append(jnp.sum(jnp.where(here, through, 0.0), axis=0, keepdims=True))
        level_rows.append(mine)
    d_local = dot_left((jnp.concatenate(highs, axis=0), jnp.concatenate(lows, axis=0)), k)
    for i, h in enumerate(heads):
        lead = halves(entry[:, h : h + 1] * residuals[i])
        d_qt = halves(d_local[i * rows : (i + 1) * rows] + dot_f32(lead, halves(comb_ref[h]), NT))
        grad_k = dot_f32(d_qt, halves(qp_ref[h]), TN)
        d_qp = dot_f32(d_qt, halves(kmap_ref[h]))
        grad_q = dot_right(q_ref[:, h * dim : (h + 1) * dim], halves(d_qp), TN)
        d_comb = dot_f32(halves(qt_ref[h]), lead, TN)
        for level in range(span_bits):
            level_rows[i].append(jnp.sum(state_ref[level, h] * d_comb, axis=0, keepdims=True))
        level_rows[i].append(jnp.zeros((pad - levels, rows), F32))
        at = pl.ds(pl.multiple_of(chunk_of(i, share, span, splits) * dim, dim), dim)
        keep_ref[at, :] = jnp.where(first, grad_q, grad_k)
        send_ref[at, :] = jnp.where(first, grad_k, grad_q)
    table = jnp.sum(jnp.concatenate([r for mine in level_rows for r in mine], axis=0), axis=1, keepdims=True)
    spread = iota2((share * pad, rows), 0) % pad == iota2((share * pad, rows), 1)
    pick = iota2((share, share * pad), 1) // pad == iota2((share, share * pad), 0)
    level_sums = exact_dot(pick.astype(F32), jnp.where(spread, table, 0.0))
    small = jnp.concatenate(gain_rows + [level_sums], axis=0)
    tail = pl.ds(share * dim, 2 * share)
    keep_ref[tail, :] = small
    send_ref[tail, :] = small


def place_kernel(span_ref, *refs, orders):
    q_ref, k_ref, level_ref, gain_ref = refs[-4:]
    heads, dim, _ = q_ref.shape
    parts = len(orders)
    share = heads // parts
    span = span_ref[0]
    first = (span & 1) == 0
    for part, splits in enumerate(orders):
        mine_ref, other_ref, small_ref = refs[3 * part : 3 * part + 3]
        tail = small_ref.shape[0] - 2 * share
        for i in range(share):
            h = part * share + i
            at = pl.ds(pl.multiple_of(chunk_of(i, share, span, splits) * dim, dim), dim)
            mine, other = mine_ref[at, :], other_ref[at, :]
            q_ref[h] = jnp.where(first, mine, other)
            k_ref[h] = jnp.where(first, other, mine)
        heads_here = pl.ds(part * share, share)
        gain_ref[heads_here, :] = small_ref[tail : tail + share, :]
        level_ref[heads_here, :] = small_ref[tail + share :, : level_ref.shape[1]]


def vmem(count):
    return [pl.BlockSpec(memory_space=pltpu.VMEM)] * count


def hbm(count):
    return [pl.BlockSpec(memory_space=pltpu.HBM)] * count


def smem(count):
    return [pl.BlockSpec(memory_space=pltpu.SMEM)] * count


def shape(*dims, dtype=F32):
    return jax.ShapeDtypeStruct(dims, dtype)


def call(kernel, ins, outs, limit, flops, scratch=(), **static):
    body = functools.partial(kernel, **static) if static else kernel
    single = not isinstance(outs, (list, tuple))
    return pl.pallas_call(
        body,
        out_shape=outs,
        in_specs=ins,
        out_specs=pl.BlockSpec(memory_space=pltpu.VMEM) if single else vmem(len(outs)),
        scratch_shapes=list(scratch),
        compiler_params=pltpu.CompilerParams(vmem_limit_bytes=limit << 20),
        cost_estimate=pl.CostEstimate(flops=flops, bytes_accessed=1 << 20, transcendentals=0),
    )


def in_hbm(*values):
    return [pltpu.with_memory_space_constraint(value, pltpu.HBM) for value in values]


def swap(value, axis, stride):
    count = lax.axis_size(axis)
    return lax.ppermute(value, axis, [(i, i ^ stride) for i in range(count)])


def on_device(queries, key_vectors, value_vectors, log_gate, query_map, key_map, level_weight, norm_gain):
    rows, dim = key_vectors.shape
    heads = queries.shape[1] // dim
    count = lax.axis_size("seq")
    groups = lax.axis_size("head")
    span_bits = count.bit_length() - 1
    span = lax.axis_index("seq").astype(jnp.int32).reshape(1)
    total_tokens = rows * count
    norm_width = heads * dim * groups
    gain = norm_gain.reshape(heads, dim)
    strides = [1 << bit for bit in reversed(range(1, span_bits))]
    orders = [(2, 4), (4, 2)]
    cube = (heads, dim, dim)
    packed_rows = 2 * rows + GATE_ROWS

    offsets = [0]
    for stride in strides:
        offsets += [offset + stride for offset in offsets]
    early = len(offsets) // 2

    packed = call(pack_kernel, hbm(3), shape(packed_rows, rows, dtype=BF16), 8, 1 << 20, scratch=[
        pltpu.VMEM((rows, dim), BF16),
        pltpu.VMEM((rows, dim), BF16),
        pltpu.VMEM((heads, rows), F32),
        pltpu.SemaphoreType.DMA((3,)),
    ])(*in_hbm(key_vectors, value_vectors, log_gate))
    qp, qt, score_decay, mix, local = call(
        local_kernel, vmem(1) + hbm(4), [shape(*cube)] * 5, 24, 1 << 29,
        scratch=[
            pltpu.VMEM(queries.shape, BF16),
            pltpu.VMEM(cube, F32),
            pltpu.VMEM(cube, F32),
            pltpu.SMEM(level_weight.shape, F32),
            pltpu.SemaphoreType.DMA((4,)),
        ],
    )(packed, *in_hbm(level_weight, queries, query_map, key_map))

    even_a = packed[None]
    for stride in strides[:-1]:
        received = swap(even_a, "seq", stride)
        even_a = jnp.concatenate([even_a, received], axis=0)
    even_b = swap(even_a, "seq", strides[-1])
    odd_a = swap(even_a, "seq", 1)
    odd_b = swap(even_b, "seq", 1)

    scores, peaks, states, ends, before = call(
        early_kernel,
        smem(1) + vmem(3),
        [
            shape(early, heads * rows, 2 * rows),
            shape(heads * rows, rows),
            shape(early, *cube),
            shape(early * heads, rows),
            shape(heads, rows),
        ],
        24,
        1 << 30,
        scratch=[pltpu.VMEM((early, heads, 2 * rows), F32)],
        offsets=tuple(offsets),
    )(span, queries, even_a, odd_a)
    raw, target, level_states, combined, sums = call(
        forward_kernel,
        smem(2) + vmem(14),
        [shape(*cube), shape(*cube), shape(span_bits, *cube), shape(*cube), shape(8, rows)],
        32,
        1 << 31,
        scratch=[
            pltpu.VMEM((early, heads * rows, 2 * rows), F32),
            pltpu.VMEM((heads * rows, rows), F32),
            pltpu.VMEM((early, *cube), F32),
            pltpu.VMEM((heads * rows, rows), F32),
            pltpu.VMEM((heads * rows, dim), F32),
        ],
        offsets=tuple(offsets),
    )(
        span, level_weight, queries, even_a, odd_a, even_b, odd_b, scores, peaks, states, ends, before,
        qt, local, gain, log_gate,
    )

    stride = 1
    while stride < groups:
        received = swap(sums, "head", stride)
        if 2 * stride < groups:
            sums = sums + received
        stride *= 2

    share = heads // PARTS
    size = share * dim
    held = []
    for part in range(PARTS):
        keep, send = call(
            backward_kernel,
            smem(1) + vmem(16),
            [shape(share * (dim + 2), dim)] * 2,
            24,
            1 << 29,
            norm_width=float(norm_width),
            total_tokens=float(total_tokens),
            splits=orders[part],
            heads=range(part * share, (part + 1) * share),
        )(
            span, sums, received, log_gate, queries, key_vectors, value_vectors, key_map, gain,
            qp, qt, score_decay, mix, raw, target, level_states, combined,
        )
        held.append(keep + swap(send, "seq", 1))
    for step in range(len(orders[0])):
        size //= 2
        for part in range(PARTS):
            split = orders[part][step]
            here = held[part]
            got = swap(here[size:], "seq", split)
            held[part] = jnp.concatenate([here[:size] + got[:size], here[2 * size :] + got[size:]])
    for stride in strides:
        if stride not in orders[0]:
            for part in range(PARTS):
                held[part] = held[part] + swap(held[part], "seq", stride)
    mine = [here[:size] for here in held]
    for step in reversed(range(len(orders[0]))):
        for part in range(PARTS):
            split = orders[part][step]
            mine[part] = jnp.concatenate([mine[part], swap(mine[part], "seq", split)])
    pieces = []
    for part in range(PARTS):
        pieces += [mine[part], swap(mine[part], "seq", 1), held[part]]
    grad_query, grad_key, grad_levels, grad_gain = call(
        place_kernel,
        smem(1) + vmem(3 * PARTS),
        [shape(*cube), shape(*cube), shape(*level_weight.shape), shape(heads, dim)],
        16,
        1 << 20,
        orders=orders,
    )(span, *pieces)
    grad_gain = grad_gain.reshape(-1)
    return grad_query, grad_key, grad_levels, grad_gain


def solution(mesh):
    placed = (
        P("seq", "head"),
        P("seq", "head"),
        P("seq", "head"),
        P("head", "seq"),
        P("head", None, None),
        P("head", None, None),
        P("head", None),
        P("head"),
    )

    return jax.shard_map(
        on_device,
        mesh=mesh,
        in_specs=placed,
        out_specs=(P("head", None, None), P("head", None, None), P("head", None), P("head")),
        check_vma=False,
    )
```

```python
import functools

import jax
import jax.numpy as jnp
from jax import lax
from jax.experimental import pallas as pl
from jax.experimental.pallas import tpu as pltpu
from jax.sharding import PartitionSpec as P


HIGHEST = lax.Precision.HIGHEST
NEGATIVE = -1e30
EPSILON = 1e-05
F32 = jnp.float32
BF16 = jnp.bfloat16
NN = (((1,), (0,)), ((), ()))
NT = (((1,), (1,)), ((), ()))
TN = (((0,), (0,)), ((), ()))
PARTS = 2


def dot(a, b, dims=NN):
    return lax.dot_general(a, b, dims, preferred_element_type=F32)


def exact_dot(a, b, dims=NN):
    return lax.dot_general(a, b, dims, precision=HIGHEST, preferred_element_type=F32)


def halves(x):
    high = x.astype(BF16)
    return high, (x - high.astype(F32)).astype(BF16)


def dot_f32(a, b, dims=NN):
    lhs = jnp.concatenate([a[0], a[0], a[1]], axis=dims[0][0][0])
    rhs = jnp.concatenate([b[0], b[1], b[0]], axis=dims[0][1][0])
    return dot(lhs, rhs, dims)


def dot_left(a, b, dims=NN):
    lhs = jnp.concatenate([a[0], a[1]], axis=dims[0][0][0])
    rhs = jnp.concatenate([b, b], axis=dims[0][1][0])
    return dot(lhs, rhs, dims)


def dot_right(a, b, dims=NN):
    lhs = jnp.concatenate([a, a], axis=dims[0][0][0])
    rhs = jnp.concatenate([b[0], b[1]], axis=dims[0][1][0])
    return dot(lhs, rhs, dims)


def iota2(shape, axis):
    return lax.broadcasted_iota(jnp.int32, shape, axis)


def upper_ones(size):
    return (iota2((size, size), 0) <= iota2((size, size), 1)).astype(F32)


def fetch(sems, *pairs):
    copies = [pltpu.make_async_copy(src, dst, sems.at[i]) for i, (src, dst) in enumerate(pairs)]
    for copy in copies:
        copy.start()
    for copy in copies:
        copy.wait()


def pack_kernel(k_hbm, v_hbm, gate_hbm, out_ref, k_ref, v_ref, gate_ref, sems):
    fetch(sems, (k_hbm, k_ref), (v_hbm, v_ref), (gate_hbm, gate_ref))
    half = k_ref.shape[0] // 2
    gate = gate_ref[...]
    high = gate.astype(BF16).astype(F32)
    middle = (gate - high).astype(BF16).astype(F32)
    gates = jnp.concatenate([high, middle, gate - high - middle], axis=0).astype(BF16)
    for part in range(2):
        tokens = slice(part * half, (part + 1) * half)
        out_ref[part, 0, 0:half, :] = k_ref[tokens, :]
        out_ref[part, 0, half : 2 * half, :] = v_ref[tokens, :]
        out_ref[part, 0, 2 * half :, :] = gates


def gates_of(piece):
    heads = piece.shape[0] // 3
    piece = piece.astype(F32)
    return piece[0:heads] + piece[heads : 2 * heads] + piece[2 * heads : 3 * heads]


def local_kernel(
    packed_ref, level_hbm, q_hbm, qmap_hbm, kmap_hbm, qp_ref, qt_ref, sd_ref, mix_ref, loc_ref, entry_ref, rows_ref,
    q_ref, qmap_ref, kmap_ref, level_ref, sems,
):
    fetch(sems, (q_hbm, q_ref), (qmap_hbm, qmap_ref), (kmap_hbm, kmap_ref), (level_hbm, level_ref))
    heads, dim, _ = qmap_ref.shape
    rows = q_ref.shape[0]
    half = rows // 2
    low_bits = rows.bit_length() - 1
    cum = exact_dot(gates_of(packed_ref[0, 0, rows:, :]), upper_ones(rows))
    cum_t = cum.T
    entry_ref[...] = jnp.exp(cum_t)
    rows_ref[...] = stacked_queries(q_ref, dim)
    k = jnp.concatenate([packed_ref[0, 0, 0:half, :], packed_ref[1, 0, 0:half, :]], axis=0)
    v = jnp.concatenate([packed_ref[0, 0, half:rows, :], packed_ref[1, 0, half:rows, :]], axis=0)
    row, col = iota2((rows, rows), 0), iota2((rows, rows), 1)
    causal = col <= row
    differ = row ^ col
    highs, lows = [], []
    for h in range(heads):
        qp = dot_right(q_ref[:, h * dim : (h + 1) * dim], halves(qmap_ref[h]))
        qp_ref[h] = qp
        qt = dot_f32(halves(qp), halves(kmap_ref[h]), NT)
        qt_ref[h] = qt
        high, low = halves(qt)
        highs.append(high)
        lows.append(low)
    score = dot_left((jnp.concatenate(highs, axis=0), jnp.concatenate(lows, axis=0)), k, NT)
    highs, lows = [], []
    for h in range(heads):
        decay = jnp.exp(jnp.where(causal, cum_t[:, h : h + 1] - cum[h : h + 1, :], NEGATIVE))
        weight = jnp.full((rows, rows), level_ref[h, 0], F32)
        for level in range(1, low_bits + 1):
            weight = jnp.where(differ >= (1 << (level - 1)), level_ref[h, level], weight)
        decayed = score[h * rows : (h + 1) * rows] * decay
        mix_ref[h] = decay * weight
        sd_ref[h] = decayed
        high, low = halves(decayed * weight)
        highs.append(high)
        lows.append(low)
    loc = dot_left((jnp.concatenate(highs, axis=0), jnp.concatenate(lows, axis=0)), v)
    for h in range(heads):
        loc_ref[h] = loc[h * rows : (h + 1) * rows]


def stacked_queries(q_ref, dim):
    return jnp.concatenate([q_ref[:, at : at + dim] for at in range(0, q_ref.shape[1], dim)], axis=0)


def unit_decay(span, evens, odds):
    gates = []
    for ref in (*evens, *odds):
        for p in range(ref.shape[0]):
            gates.append(gates_of(ref[p, ref.shape[2] :, :]))
    rows = gates[0].shape[1]
    cum = exact_dot(jnp.concatenate(gates, axis=0), upper_ones(rows))
    end = jnp.broadcast_to(cum[:, rows - 1 : rows], cum.shape)
    size = cum.shape[0] // 4
    odd_span = (span & 1) == 1
    units, nexts = [], []
    left = iota2((size, rows), 1) < rows // 2
    for part in range(2):
        e, o = slice(part * size, (part + 1) * size), slice((part + 2) * size, (part + 3) * size)
        decay_e = jnp.exp(end[e] - cum[e] + jnp.where(odd_span, 0.0, end[o]))
        decay_o = jnp.exp(end[o] - cum[o] + jnp.where(odd_span, end[e], 0.0))
        alone = jnp.exp(end[o] - cum[o])
        if part == 0:
            decay_o, alone = pltpu.roll(decay_o, rows // 2, 1), pltpu.roll(alone, rows // 2, 1)
        else:
            decay_e = pltpu.roll(decay_e, rows // 2, 1)
        units.append(jnp.where(left, decay_e, decay_o))
        nexts.append(jnp.where(left, 0.0, alone))
    return units, nexts, end[0:size] + end[2 * size : 3 * size], end[2 * size : 3 * size]


def unit_block(even_ref, odd_ref, p):
    half = even_ref.shape[2] // 2
    k = jnp.concatenate([even_ref[p, 0:half, :], odd_ref[p, 0:half, :]], axis=0)
    v = jnp.concatenate([even_ref[p, half : 2 * half, :], odd_ref[p, half : 2 * half, :]], axis=0)
    return k.astype(F32).T, v


def unit_values(even_ref, odd_ref, p):
    half = even_ref.shape[2] // 2
    return [even_ref[p, half : 2 * half, :], odd_ref[p, half : 2 * half, :]]


def pair_state(kt, v, weight, state_ref, i):
    heads = weight.shape[0]
    dim = kt.shape[0]
    highs, lows = [], []
    for h in range(heads):
        high, low = halves(kt * weight[h : h + 1, :])
        highs.append(high)
        lows.append(low)
    state = dot_left((jnp.concatenate(highs, axis=0), jnp.concatenate(lows, axis=0)), v)
    for h in range(heads):
        state_ref[i, h] = state[h * dim : (h + 1) * dim]


def pairs_of(offsets):
    table = {}
    for part, row in enumerate(offsets):
        for p, offset in enumerate(row):
            table.setdefault(offset, []).append((part, p))
    return sorted(table.items())


def by_level(table):
    levels = {}
    for i, (offset, units) in enumerate(table):
        if offset:
            levels.setdefault(offset.bit_length() - 1, []).append((i, units))
    return sorted(levels.items())


def take_level(group, q_all, evens, odds, weights, score_ref, peak_ref, state_ref):
    heads = q_all.shape[0] // evens[0].shape[2]
    count = evens[0].shape[0]
    scale = q_all.shape[1] ** (-0.5)
    blocks = {unit: unit_block(evens[unit[0]], odds[unit[0]], unit[1]) for _, units in group for unit in units}
    top = peak_ref[...]
    names = list(blocks)
    for at in range(0, len(names), 2):
        both = names[at : at + 2]
        keys = jnp.concatenate([blocks[unit][0].astype(BF16) for unit in both], axis=1)
        score = dot(q_all, keys) * scale
        for i, (part, p) in enumerate(both):
            one = score[:, i * (score.shape[1] // len(both)) : (i + 1) * (score.shape[1] // len(both))]
            score_ref[part * count + p] = one
            top = jnp.maximum(top, one)
    peak_ref[...] = top
    for i, units in group:
        kt = jnp.concatenate([blocks[unit][0] for unit in units], axis=1)
        v = jnp.concatenate([blocks[unit][1] for unit in units], axis=0)
        weight = jnp.concatenate([weights[part][p * heads : (p + 1) * heads] for part, p in units], axis=1)
        pair_state(kt, v, weight, state_ref, i)


def early_kernel(
    span_ref, q_ref, even_a_ref, odd_a_ref, even_b_ref, odd_b_ref,
    score_ref, peak_ref, state_ref, ends_ref, before_ref, *, offsets,
):
    _, heads, dim, _ = state_ref.shape
    rows = even_a_ref.shape[2]
    span = span_ref[0]
    evens, odds = (even_a_ref, even_b_ref), (odd_a_ref, odd_b_ref)
    weights, nexts, ends, later = unit_decay(span, evens, odds)
    ends_ref[...] = ends
    before_ref[...] = later[0:heads]
    q_all = q_ref[...]
    count = even_a_ref.shape[0]
    table = pairs_of(offsets)
    odd_span = (span & 1) == 1
    row, col = iota2((rows, 2 * rows), 0), iota2((rows, 2 * rows), 1)
    place = col % rows
    token = place + (col // rows) * (rows // 2)
    seen = ((place < rows // 2) & (token <= row)) | ((place >= rows // 2) & odd_span)
    blocks = [unit_block(evens[part], odds[part], 0) for part in range(2)]
    kt = jnp.concatenate([kt for kt, _ in blocks], axis=1)
    score = dot(q_all, kt.astype(BF16)) * dim ** (-0.5)
    score = jnp.where(jnp.concatenate([seen] * heads, axis=0), score, NEGATIVE)
    score_ref[0] = score[:, :rows]
    score_ref[count] = score[:, rows:]
    peak_ref[...] = jnp.maximum(score[:, :rows], score[:, rows:])

    @pl.when(odd_span)
    def _():
        v = jnp.concatenate([v for _, v in blocks], axis=0)
        pair_state(kt, v, jnp.concatenate([nexts[0][0:heads], nexts[1][0:heads]], axis=1), state_ref, 0)

    for bit, group in by_level(table):

        @pl.when(((span >> bit) & 1) == 1)
        def _(group=group):
            take_level(group, q_all, evens, odds, weights, score_ref, peak_ref, state_ref)


def forward_kernel(
    span_ref, level_ref, q_ref, ea_ref, oa_ref, eb_ref, ob_ref, late_ea_ref, late_oa_ref, late_eb_ref, late_ob_ref,
    score_a_ref, peak_a_ref, state_a_ref, ends_a_ref, before_ref, qt_ref, loc_ref, gain_ref, entry_ref,
    raw_ref, target_ref, level_state_ref, comb_ref, sums_ref,
    score_scr, peak_scr, state_scr, total_scr, acc_scr, *, early, late,
):
    heads, rows, dim = qt_ref.shape
    count = ea_ref.shape[0]
    offsets = early[0] + late[0]
    pairs = len(offsets)
    span_bits = level_state_ref.shape[0]
    low_bits = rows.bit_length() - 1
    span = span_ref[0]
    odd_span = (span & 1) == 1
    q_all = q_ref[...]
    early_refs = ((ea_ref, eb_ref), (oa_ref, ob_ref))
    late_refs = ((late_ea_ref, late_eb_ref), (late_oa_ref, late_ob_ref))
    early_table, late_table = pairs_of(early), pairs_of(late)
    weights, _, ends_b, _ = unit_decay(span, *late_refs)
    peak_scr[...] = peak_a_ref[...]
    for bit, group in by_level(late_table):

        @pl.when(((span >> bit) & 1) == 1)
        def _(group=group):
            take_level(group, q_all, *late_refs, weights, score_scr, peak_scr, state_scr)

    ends = jnp.concatenate([ends_a_ref[...], ends_b], axis=0)
    size = pairs * heads

    def pair_of(index):
        position = index // heads
        offset = position * 0
        for p in range(pairs):
            offset = jnp.where(position == p, offsets[p], offset)
        return (span ^ offset) >> 1, index % heads

    mine, my_head = pair_of(iota2((size, size), 0))
    other, other_head = pair_of(iota2((size, size), 1))
    between = (other > mine) & (other < (span >> 1)) & (my_head == other_head)
    carried = exact_dot(between.astype(F32), ends)
    before = jnp.where(odd_span, before_ref[...], 0.0)
    factor = jnp.exp(carried + jnp.concatenate([before] * pairs, axis=0))

    peak = jnp.max(peak_scr[...], axis=1, keepdims=True)
    peak_scr[...] = jnp.broadcast_to(peak, peak_scr.shape)

    def weigh(early_units, late_units):
        top = peak_scr[...]
        total, parts, values = None, [], []
        for units, refs, score_ref in ((early_units, early_refs, score_a_ref), (late_units, late_refs, score_scr)):
            for part, p in units:
                weight = jnp.exp(score_ref[part * count + p] - top)
                total = weight if total is None else total + weight
                parts.append(weight.astype(BF16))
                values += unit_values(refs[0][part], refs[1][part], p)
        return total, dot(jnp.concatenate(parts, axis=1), jnp.concatenate(values, axis=0))

    total_scr[...], acc_scr[...] = weigh([(0, 0), (1, 0)], [])
    early_levels, late_levels = dict(by_level(early_table)), dict(by_level(late_table))
    for bit in sorted({*early_levels, *late_levels}):

        @pl.when(((span >> bit) & 1) == 1)
        def _(bit=bit):
            total, acc = weigh(
                [unit for _, units in early_levels.get(bit, []) for unit in units],
                [unit for _, units in late_levels.get(bit, []) for unit in units],
            )
            total_scr[...] += total
            acc_scr[...] += acc

    for level in range(span_bits):
        used = ((span >> level) & 1) == 1
        members = [
            (ref, i, offset)
            for ref, table in ((state_a_ref, early_table), (state_scr, late_table))
            for i, (offset, _) in enumerate(table)
            if max(offset, 1).bit_length() - 1 == level
        ]

        @pl.when(used)
        def _(members=members, level=level):
            for h in range(heads):
                value = None
                for ref, i, offset in members:
                    state = ref[i, h]
                    if offset:
                        at = offsets.index(offset) * heads + h
                        state = state * factor[at : at + 1, :]
                    value = state if value is None else value + state
                level_state_ref[level, h] = value

        @pl.when(jnp.logical_not(used))
        def _(level=level):
            level_state_ref[level] = jnp.zeros_like(level_state_ref[level])

    total = jnp.sum(total_scr[...], axis=1, keepdims=True)
    target_all = acc_scr[...] / total
    entry = entry_ref[...]
    squares = jnp.zeros((rows, dim), F32)
    gained = jnp.zeros((rows, dim), F32)
    crossed = jnp.zeros((rows, dim), F32)
    for h in range(heads):
        combined = jnp.zeros((dim, dim), F32)
        for level in range(span_bits):
            combined = combined + level_ref[h, low_bits + 1 + level] * level_state_ref[level, h]
        comb_ref[h] = combined
        far = entry[:, h : h + 1] * dot_f32(halves(qt_ref[h]), halves(combined))
        raw = loc_ref[h] + far
        target = target_all[h * rows : (h + 1) * rows]
        raw_ref[h] = raw
        target_ref[h] = target
        gain = gain_ref[h : h + 1, :]
        square = raw * raw
        squares = squares + square
        gained = gained + square * (gain * gain)
        crossed = crossed + target * raw * gain
    lanes = iota2((rows, rows), 1)
    columns = jnp.where(
        lanes == 0,
        jnp.sum(squares, axis=1, keepdims=True),
        jnp.where(
            lanes == 1,
            jnp.sum(gained, axis=1, keepdims=True),
            jnp.where(lanes == 2, jnp.sum(crossed, axis=1, keepdims=True), 0.0),
        ),
    )
    sums_ref[...] = columns.T[0:8]


def chunk_of(head, heads, span, splits):
    group = heads >> len(splits)
    chunk = 0
    for place, stride in enumerate(splits):
        shift = len(splits) - 1 - place
        bit = (head // group >> shift) & 1
        chunk = chunk + ((bit ^ ((span // stride) & 1)) << shift)
    return chunk * group + head % group


def backward_kernel(
    span_ref, sums_a_ref, sums_b_ref, entry_ref, q_ref, k_ref, v_ref, kmap_ref, gain_ref,
    qp_ref, qt_ref, sd_ref, mix_ref, raw_ref, target_ref, state_ref, comb_ref,
    keep_ref, send_ref, *, norm_width, total_tokens, splits, heads,
):
    _, rows, dim = qt_ref.shape
    share = len(heads)
    span_bits = state_ref.shape[0]
    low_bits = rows.bit_length() - 1
    span = span_ref[0]
    first = (span & 1) == 0
    sums = (sums_a_ref[...] + sums_b_ref[...]).T
    squares, gained, crossed = sums[:, 0:1], sums[:, 1:2], sums[:, 2:3]
    inverse = lax.rsqrt(squares / norm_width + EPSILON)
    inner = (inverse * gained - crossed) / total_tokens
    shrink = inverse * inverse * inverse * inner / norm_width
    entry = entry_ref[...]
    k = k_ref[...]
    v = v_ref[...]
    row, col = iota2((rows, rows), 0), iota2((rows, rows), 1)
    differ = row ^ col
    levels = low_bits + 1 + span_bits
    pad = 16
    gain_rows, residuals, highs, lows = [], [], [], []
    for h in heads:
        gain = gain_ref[h : h + 1, :]
        raw = raw_ref[h]
        normed = raw * inverse
        mismatch = (normed * gain - target_ref[h]) / total_tokens
        gain_rows.append(jnp.sum(mismatch * normed, axis=0, keepdims=True))
        residual = inverse * (mismatch * gain) - raw * shrink
        residuals.append(residual)
        high, low = halves(residual)
        highs.append(high)
        lows.append(low)
    d_mix = dot_left((jnp.concatenate(highs, axis=0), jnp.concatenate(lows, axis=0)), v, NT)
    level_rows, highs, lows = [], [], []
    for i, h in enumerate(heads):
        d_mix_h = d_mix[i * rows : (i + 1) * rows]
        high, low = halves(d_mix_h * mix_ref[h])
        highs.append(high)
        lows.append(low)
        through = d_mix_h * sd_ref[h]
        mine = []
        for level in range(low_bits + 1):
            least = 0 if level == 0 else 1 << (level - 1)
            here = (differ >= least) & (differ < (1 << level))
            mine.append(jnp.sum(jnp.where(here, through, 0.0), axis=0, keepdims=True))
        level_rows.append(mine)
    d_local = dot_left((jnp.concatenate(highs, axis=0), jnp.concatenate(lows, axis=0)), k)
    for i, h in enumerate(heads):
        lead = halves(entry[:, h : h + 1] * residuals[i])
        d_qt = halves(d_local[i * rows : (i + 1) * rows] + dot_f32(lead, halves(comb_ref[h]), NT))
        grad_k = dot_f32(d_qt, halves(qp_ref[h]), TN)
        d_qp = dot_f32(d_qt, halves(kmap_ref[h]))
        grad_q = dot_right(q_ref[h * rows : (h + 1) * rows, :], halves(d_qp), TN)
        d_comb = dot_f32(halves(qt_ref[h]), lead, TN)
        for level in range(span_bits):
            level_rows[i].append(jnp.sum(state_ref[level, h] * d_comb, axis=0, keepdims=True))
        level_rows[i].append(jnp.zeros((pad - levels, rows), F32))
        at = pl.ds(pl.multiple_of(chunk_of(i, share, span, splits) * dim, dim), dim)
        keep_ref[at, :] = jnp.where(first, grad_q, grad_k)
        send_ref[at, :] = jnp.where(first, grad_k, grad_q)
    table = jnp.sum(jnp.concatenate([r for mine in level_rows for r in mine], axis=0), axis=1, keepdims=True)
    spread = iota2((share * pad, rows), 0) % pad == iota2((share * pad, rows), 1)
    pick = iota2((share, share * pad), 1) // pad == iota2((share, share * pad), 0)
    level_sums = exact_dot(pick.astype(F32), jnp.where(spread, table, 0.0))
    small = jnp.concatenate(gain_rows + [level_sums], axis=0)
    tail = pl.ds(share * dim, 2 * share)
    keep_ref[tail, :] = small
    send_ref[tail, :] = small


def place_kernel(span_ref, *refs, orders):
    q_ref, k_ref, level_ref, gain_ref = refs[-4:]
    heads, dim, _ = q_ref.shape
    parts = len(orders)
    share = heads // parts
    span = span_ref[0]
    first = (span & 1) == 0
    for part, splits in enumerate(orders):
        mine_ref, other_ref, small_ref = refs[3 * part : 3 * part + 3]
        tail = small_ref.shape[0] - 2 * share
        for i in range(share):
            h = part * share + i
            at = pl.ds(pl.multiple_of(chunk_of(i, share, span, splits) * dim, dim), dim)
            mine, other = mine_ref[at, :], other_ref[at, :]
            q_ref[h] = jnp.where(first, mine, other)
            k_ref[h] = jnp.where(first, other, mine)
        heads_here = pl.ds(part * share, share)
        gain_ref[heads_here, :] = small_ref[tail : tail + share, :]
        level_ref[heads_here, :] = small_ref[tail + share :, : level_ref.shape[1]]


def vmem(count):
    return [pl.BlockSpec(memory_space=pltpu.VMEM)] * count


def hbm(count):
    return [pl.BlockSpec(memory_space=pltpu.HBM)] * count


def smem(count):
    return [pl.BlockSpec(memory_space=pltpu.SMEM)] * count


def shape(*dims, dtype=F32):
    return jax.ShapeDtypeStruct(dims, dtype)


def call(kernel, ins, outs, limit, flops, scratch=(), **static):
    body = functools.partial(kernel, **static) if static else kernel
    single = not isinstance(outs, (list, tuple))
    return pl.pallas_call(
        body,
        out_shape=outs,
        in_specs=ins,
        out_specs=pl.BlockSpec(memory_space=pltpu.VMEM) if single else vmem(len(outs)),
        scratch_shapes=list(scratch),
        compiler_params=pltpu.CompilerParams(vmem_limit_bytes=limit << 20),
        cost_estimate=pl.CostEstimate(flops=flops, bytes_accessed=1 << 20, transcendentals=0),
    )


def in_hbm(*values):
    return [pltpu.with_memory_space_constraint(value, pltpu.HBM) for value in values]


def swap(value, axis, stride):
    count = lax.axis_size(axis)
    return lax.ppermute(value, axis, [(i, i ^ stride) for i in range(count)])


def on_device(queries, key_vectors, value_vectors, log_gate, query_map, key_map, level_weight, norm_gain):
    rows, dim = key_vectors.shape
    heads = queries.shape[1] // dim
    count = lax.axis_size("seq")
    groups = lax.axis_size("head")
    span_bits = count.bit_length() - 1
    span = lax.axis_index("seq").astype(jnp.int32).reshape(1)
    total_tokens = rows * count
    norm_width = heads * dim * groups
    gain = norm_gain.reshape(heads, dim)
    strides = [1 << bit for bit in reversed(range(1, span_bits))]
    orders = [(2, 4), (4, 2)]
    cube = (heads, dim, dim)
    packed_rows = rows + 3 * heads

    shared, (far, near) = strides[:-2], strides[-2:]
    offsets = [0]
    for stride in shared:
        offsets += [offset + stride for offset in offsets]
    early = [offsets + [offset + turn for offset in offsets] for turn in (far, near)]
    late = [[offset + turn for offset in row] for row, turn in zip(early, (near, far))]
    count_early = len(early[0])

    packed = call(pack_kernel, hbm(3), shape(2, 1, packed_rows, dim, dtype=BF16), 8, 1 << 20, scratch=[
        pltpu.VMEM((rows, dim), BF16),
        pltpu.VMEM((rows, dim), BF16),
        pltpu.VMEM((heads, rows), F32),
        pltpu.SemaphoreType.DMA((3,)),
    ])(*in_hbm(key_vectors, value_vectors, log_gate))
    qp, qt, score_decay, mix, local, entry, stacked = call(
        local_kernel, vmem(1) + hbm(4), [shape(*cube)] * 5 + [shape(rows, heads), shape(heads * rows, dim, dtype=BF16)], 24, 1 << 29,
        scratch=[
            pltpu.VMEM(queries.shape, BF16),
            pltpu.VMEM(cube, F32),
            pltpu.VMEM(cube, F32),
            pltpu.SMEM(level_weight.shape, F32),
            pltpu.SemaphoreType.DMA((4,)),
        ],
    )(packed, *in_hbm(level_weight, queries, query_map, key_map))

    held = packed
    for stride in shared:
        received = swap(held, "seq", stride)
        held = jnp.concatenate([held, received], axis=1)
    evens, odds = [], []
    for part, turn in enumerate((far, near)):
        evens.append(jnp.concatenate([held[part], swap(held[part], "seq", turn)], axis=0))
    for part, turn in enumerate((near, far)):
        evens.append(swap(evens[part], "seq", turn))
        odds.append(swap(evens[part], "seq", 1))
    for part in range(2):
        odds.append(swap(evens[2 + part], "seq", 1))
    blocks = [value for pair in zip(evens, odds) for value in pair]

    scores, peaks, states, ends, before = call(
        early_kernel,
        smem(1) + vmem(5),
        [
            shape(2 * count_early, heads * rows, rows),
            shape(heads * rows, rows),
            shape(len(pairs_of(early)), *cube),
            shape(count_early * heads, rows),
            shape(heads, rows),
        ],
        24,
        1 << 30,
        offsets=early,
    )(span, stacked, *blocks[:4])
    raw, target, level_states, combined, sums = call(
        forward_kernel,
        smem(2) + vmem(18),
        [shape(*cube), shape(*cube), shape(span_bits, *cube), shape(*cube), shape(8, rows)],
        32,
        1 << 31,
        scratch=[
            pltpu.VMEM((2 * count_early, heads * rows, rows), F32),
            pltpu.VMEM((heads * rows, rows), F32),
            pltpu.VMEM((len(pairs_of(late)), *cube), F32),
            pltpu.VMEM((heads * rows, rows), F32),
            pltpu.VMEM((heads * rows, dim), F32),
        ],
        early=early,
        late=late,
    )(
        span, level_weight, stacked, *blocks, scores, peaks, states, ends, before, qt, local, gain, entry,
    )

    stride = 1
    while stride < groups:
        received = swap(sums, "head", stride)
        if 2 * stride < groups:
            sums = sums + received
        stride *= 2

    share = heads // PARTS
    size = share * dim
    held = []
    for part in range(PARTS):
        keep, send = call(
            backward_kernel,
            smem(1) + vmem(16),
            [shape(share * (dim + 2), dim)] * 2,
            24,
            1 << 29,
            norm_width=float(norm_width),
            total_tokens=float(total_tokens),
            splits=orders[part],
            heads=range(part * share, (part + 1) * share),
        )(
            span, sums, received, entry, stacked, key_vectors, value_vectors, key_map, gain,
            qp, qt, score_decay, mix, raw, target, level_states, combined,
        )
        held.append(keep + swap(send, "seq", 1))
    for step in range(len(orders[0])):
        size //= 2
        for part in range(PARTS):
            split = orders[part][step]
            here = held[part]
            got = swap(here[size:], "seq", split)
            held[part] = jnp.concatenate([here[:size] + got[:size], here[2 * size :] + got[size:]])
    for stride in strides:
        if stride not in orders[0]:
            for part in range(PARTS):
                held[part] = held[part] + swap(held[part], "seq", stride)
    mine = [here[:size] for here in held]
    for step in reversed(range(len(orders[0]))):
        for part in range(PARTS):
            split = orders[part][step]
            mine[part] = jnp.concatenate([mine[part], swap(mine[part], "seq", split)])
    pieces = []
    for part in range(PARTS):
        pieces += [mine[part], swap(mine[part], "seq", 1), held[part]]
    grad_query, grad_key, grad_levels, grad_gain = call(
        place_kernel,
        smem(1) + vmem(3 * PARTS),
        [shape(*cube), shape(*cube), shape(*level_weight.shape), shape(heads, dim)],
        16,
        1 << 20,
        orders=orders,
    )(span, *pieces)
    grad_gain = grad_gain.reshape(-1)
    return grad_query, grad_key, grad_levels, grad_gain


def solution(mesh):
    placed = (
        P("seq", "head"),
        P("seq", "head"),
        P("seq", "head"),
        P("head", "seq"),
        P("head", None, None),
        P("head", None, None),
        P("head", None),
        P("head"),
    )

    return jax.shard_map(
        on_device,
        mesh=mesh,
        in_specs=placed,
        out_specs=(P("head", None, None), P("head", None, None), P("head", None), P("head")),
        check_vma=False,
    )
```

```python
import functools

import jax
import jax.numpy as jnp
from jax import lax
from jax.experimental import pallas as pl
from jax.experimental.pallas import tpu as pltpu
from jax.sharding import PartitionSpec as P


HIGHEST = lax.Precision.HIGHEST
NEGATIVE = -1e30
EPSILON = 1e-05
LOG2E = 1.4426950408889634
F32 = jnp.float32
BF16 = jnp.bfloat16
NN = (((1,), (0,)), ((), ()))
NT = (((1,), (1,)), ((), ()))
TN = (((0,), (0,)), ((), ()))
PARTS = 2


def dot(a, b, dims=NN):
    return lax.dot_general(a, b, dims, preferred_element_type=F32)


def exact_dot(a, b, dims=NN):
    return lax.dot_general(a, b, dims, precision=HIGHEST, preferred_element_type=F32)


def halves(x):
    high = x.astype(BF16)
    return high, (x - high.astype(F32)).astype(BF16)


def dot_f32(a, b, dims=NN):
    lhs = jnp.concatenate([a[0], a[0], a[1]], axis=dims[0][0][0])
    rhs = jnp.concatenate([b[0], b[1], b[0]], axis=dims[0][1][0])
    return dot(lhs, rhs, dims)


def dot_left(a, b, dims=NN):
    lhs = jnp.concatenate([a[0], a[1]], axis=dims[0][0][0])
    rhs = jnp.concatenate([b, b], axis=dims[0][1][0])
    return dot(lhs, rhs, dims)


def dot_right(a, b, dims=NN):
    lhs = jnp.concatenate([a, a], axis=dims[0][0][0])
    rhs = jnp.concatenate([b[0], b[1]], axis=dims[0][1][0])
    return dot(lhs, rhs, dims)


def iota2(shape, axis):
    return lax.broadcasted_iota(jnp.int32, shape, axis)


def upper_ones(size):
    return (iota2((size, size), 0) <= iota2((size, size), 1)).astype(F32)


def fetch(sems, *pairs):
    copies = [pltpu.make_async_copy(src, dst, sems.at[i]) for i, (src, dst) in enumerate(pairs)]
    for copy in copies:
        copy.start()
    for copy in copies:
        copy.wait()


def pack_kernel(k_hbm, v_hbm, gate_hbm, out_ref, k_ref, v_ref, gate_ref, sems):
    fetch(sems, (k_hbm, k_ref), (v_hbm, v_ref), (gate_hbm, gate_ref))
    half = k_ref.shape[0] // 2
    gate = gate_ref[...]
    high = gate.astype(BF16).astype(F32)
    middle = (gate - high).astype(BF16).astype(F32)
    gates = jnp.concatenate([high, middle, gate - high - middle], axis=0).astype(BF16)
    for part in range(2):
        tokens = slice(part * half, (part + 1) * half)
        out_ref[part, 0, 0:half, :] = k_ref[tokens, :]
        out_ref[part, 0, half : 2 * half, :] = v_ref[tokens, :]
        out_ref[part, 0, 2 * half :, :] = gates


def gates_of(piece):
    heads = piece.shape[0] // 3
    piece = piece.astype(F32)
    return piece[0:heads] + piece[heads : 2 * heads] + piece[2 * heads : 3 * heads]


def local_kernel(
    packed_ref, level_hbm, q_hbm, qmap_hbm, kmap_hbm, qp_ref, qe_ref, km_ref, sd_ref, mix_ref, loc_ref, entry_ref, rows_ref,
    q_ref, qmap_ref, kmap_ref, level_ref, sems,
):
    fetch(sems, (q_hbm, q_ref), (qmap_hbm, qmap_ref), (kmap_hbm, kmap_ref), (level_hbm, level_ref))
    heads, dim, _ = qmap_ref.shape
    rows = q_ref.shape[0]
    half = rows // 2
    low_bits = rows.bit_length() - 1
    cum = exact_dot(gates_of(packed_ref[0, 0, rows:, :]), upper_ones(rows))
    cum_t = cum.T
    rows_ref[...] = stacked_queries(q_ref, dim)
    k = jnp.concatenate([packed_ref[0, 0, 0:half, :], packed_ref[1, 0, 0:half, :]], axis=0)
    v = jnp.concatenate([packed_ref[0, 0, half:rows, :], packed_ref[1, 0, half:rows, :]], axis=0)
    row, col = iota2((rows, rows), 0), iota2((rows, rows), 1)
    causal = col <= row
    differ = row ^ col
    highs, lows = [], []
    entry = jnp.exp(cum_t)
    entry_ref[...] = entry
    for h in range(heads):
        qp = halves(dot_right(q_ref[:, h * dim : (h + 1) * dim], halves(qmap_ref[h])))
        km = halves(kmap_ref[h])
        qp_ref[h, 0], qp_ref[h, 1] = qp
        km_ref[h, 0], km_ref[h, 1] = km
        qt = dot_f32(qp, km, NT)
        qe_ref[h, 0], qe_ref[h, 1] = halves(entry[:, h : h + 1] * qt)
        high, low = halves(qt)
        highs.append(high)
        lows.append(low)
    score = dot_left((jnp.concatenate(highs, axis=0), jnp.concatenate(lows, axis=0)), k, NT)
    highs, lows = [], []
    for h in range(heads):
        decay = jnp.exp(jnp.where(causal, cum_t[:, h : h + 1] - cum[h : h + 1, :], NEGATIVE))
        weight = jnp.full((rows, rows), level_ref[h, 0], F32)
        for level in range(1, low_bits + 1):
            weight = jnp.where(differ >= (1 << (level - 1)), level_ref[h, level], weight)
        decayed = score[h * rows : (h + 1) * rows] * decay
        mix_ref[h] = decay * weight
        sd_ref[h] = decayed
        high, low = halves(decayed * weight)
        highs.append(high)
        lows.append(low)
    loc = dot_left((jnp.concatenate(highs, axis=0), jnp.concatenate(lows, axis=0)), v)
    for h in range(heads):
        loc_ref[h] = loc[h * rows : (h + 1) * rows]


def stacked_queries(q_ref, dim):
    return jnp.concatenate([q_ref[:, at : at + dim] for at in range(0, q_ref.shape[1], dim)], axis=0)


def unit_decay(span, evens, odds):
    gates = []
    for ref in (*evens, *odds):
        for p in range(ref.shape[0]):
            gates.append(gates_of(ref[p, ref.shape[2] :, :]))
    rows = gates[0].shape[1]
    cum = exact_dot(jnp.concatenate(gates, axis=0), upper_ones(rows))
    end = jnp.broadcast_to(cum[:, rows - 1 : rows], cum.shape)
    size = cum.shape[0] // 4
    odd_span = (span & 1) == 1
    units, nexts = [], []
    left = iota2((size, rows), 1) < rows // 2
    for part in range(2):
        e, o = slice(part * size, (part + 1) * size), slice((part + 2) * size, (part + 3) * size)
        decay_e = jnp.exp(end[e] - cum[e] + jnp.where(odd_span, 0.0, end[o]))
        decay_o = jnp.exp(end[o] - cum[o] + jnp.where(odd_span, end[e], 0.0))
        alone = jnp.exp(end[o] - cum[o])
        if part == 0:
            decay_o, alone = pltpu.roll(decay_o, rows // 2, 1), pltpu.roll(alone, rows // 2, 1)
        else:
            decay_e = pltpu.roll(decay_e, rows // 2, 1)
        units.append(jnp.where(left, decay_e, decay_o))
        nexts.append(jnp.where(left, 0.0, alone))
    return units, nexts, end[0:size] + end[2 * size : 3 * size], end[2 * size : 3 * size]


def unit_block(even_ref, odd_ref, p):
    half = even_ref.shape[2] // 2
    k = jnp.concatenate([even_ref[p, 0:half, :], odd_ref[p, 0:half, :]], axis=0)
    v = jnp.concatenate([even_ref[p, half : 2 * half, :], odd_ref[p, half : 2 * half, :]], axis=0)
    return k.astype(F32).T, v


def unit_values(even_ref, odd_ref, p):
    half = even_ref.shape[2] // 2
    return [even_ref[p, half : 2 * half, :], odd_ref[p, half : 2 * half, :]]


def pair_state(kt, v, weight, state_ref, i, base_ref=None, base=0):
    heads = weight.shape[0]
    dim = kt.shape[0]
    highs, lows = [], []
    for h in range(heads):
        high, low = halves(kt * weight[h : h + 1, :])
        highs.append(high)
        lows.append(low)
    state = dot_left((jnp.concatenate(highs, axis=0), jnp.concatenate(lows, axis=0)), v)
    for h in range(heads):
        value = state[h * dim : (h + 1) * dim]
        state_ref[i, h] = value if base_ref is None else value + base_ref[base, h]


def pairs_of(offsets):
    table = {}
    for part, row in enumerate(offsets):
        for p, offset in enumerate(row):
            table.setdefault(offset, []).append((part, p))
    return sorted(table.items())


def by_level(table):
    levels = {}
    for i, (offset, units) in enumerate(table):
        if offset:
            levels.setdefault(offset.bit_length() - 1, []).append((i, units))
    return sorted(levels.items())


def take_level(group, q_all, evens, odds, weights, score_ref, peak_ref, state_ref, base_ref=None, bases={}):
    heads = q_all.shape[0] // evens[0].shape[2]
    count = evens[0].shape[0]
    scale = LOG2E * q_all.shape[1] ** (-0.5)
    blocks = {unit: unit_block(evens[unit[0]], odds[unit[0]], unit[1]) for _, units in group for unit in units}
    top = peak_ref[...]
    names = list(blocks)
    for at in range(0, len(names), 2):
        both = names[at : at + 2]
        keys = jnp.concatenate([blocks[unit][0].astype(BF16) for unit in both], axis=1)
        score = dot(q_all, keys) * scale
        for i, (part, p) in enumerate(both):
            one = score[:, i * (score.shape[1] // len(both)) : (i + 1) * (score.shape[1] // len(both))]
            score_ref[part * count + p] = one
            top = jnp.maximum(top, one)
    peak_ref[...] = top
    for i, units in group:
        kt = jnp.concatenate([blocks[unit][0] for unit in units], axis=1)
        v = jnp.concatenate([blocks[unit][1] for unit in units], axis=0)
        weight = jnp.concatenate([weights[part][p * heads : (p + 1) * heads] for part, p in units], axis=1)
        pair_state(kt, v, weight, state_ref, i, base_ref if i in bases else None, bases.get(i, 0))


def early_kernel(
    span_ref, q_ref, even_a_ref, odd_a_ref, even_b_ref, odd_b_ref,
    score_ref, peak_ref, state_ref, ends_ref, before_ref, *, offsets,
):
    _, heads, dim, _ = state_ref.shape
    rows = even_a_ref.shape[2]
    span = span_ref[0]
    evens, odds = (even_a_ref, even_b_ref), (odd_a_ref, odd_b_ref)
    weights, nexts, ends, later = unit_decay(span, evens, odds)
    ends_ref[...] = ends
    before_ref[...] = later[0:heads]
    q_all = q_ref[...]
    count = even_a_ref.shape[0]
    table = pairs_of(offsets)
    odd_span = (span & 1) == 1
    row, col = iota2((rows, 2 * rows), 0), iota2((rows, 2 * rows), 1)
    place = col % rows
    token = place + (col // rows) * (rows // 2)
    seen = ((place < rows // 2) & (token <= row)) | ((place >= rows // 2) & odd_span)
    blocks = [unit_block(evens[part], odds[part], 0) for part in range(2)]
    kt = jnp.concatenate([kt for kt, _ in blocks], axis=1)
    score = dot(q_all, kt.astype(BF16)) * (LOG2E * dim ** (-0.5))
    score = jnp.where(jnp.concatenate([seen] * heads, axis=0), score, NEGATIVE)
    score_ref[0] = score[:, :rows]
    score_ref[count] = score[:, rows:]
    peak_ref[...] = jnp.maximum(score[:, :rows], score[:, rows:])

    @pl.when(odd_span)
    def _():
        v = jnp.concatenate([v for _, v in blocks], axis=0)
        pair_state(kt, v, jnp.concatenate([nexts[0][0:heads], nexts[1][0:heads]], axis=1), state_ref, 0)

    for bit, group in by_level(table):

        @pl.when(((span >> bit) & 1) == 1)
        def _(group=group):
            take_level(group, q_all, evens, odds, weights, score_ref, peak_ref, state_ref)


def forward_kernel(
    span_ref, level_ref, q_ref, ea_ref, oa_ref, eb_ref, ob_ref, late_ea_ref, late_oa_ref, late_eb_ref, late_ob_ref,
    score_a_ref, peak_a_ref, state_a_ref, ends_a_ref, before_ref, qe_ref, loc_ref, gain_ref,
    raw_ref, target_ref, level_state_ref, comb_ref, sums_ref,
    score_scr, peak_scr, state_scr, total_scr, acc_scr, *, early, late,
):
    heads, rows, dim = loc_ref.shape
    count = ea_ref.shape[0]
    offsets = early[0] + late[0]
    pairs = len(offsets)
    span_bits = level_state_ref.shape[0]
    low_bits = rows.bit_length() - 1
    span = span_ref[0]
    odd_span = (span & 1) == 1
    q_all = q_ref[...]
    early_refs = ((ea_ref, eb_ref), (oa_ref, ob_ref))
    late_refs = ((late_ea_ref, late_eb_ref), (late_oa_ref, late_ob_ref))
    early_table, late_table = pairs_of(early), pairs_of(late)
    weights, _, ends_b, _ = unit_decay(span, *late_refs)
    ends = jnp.concatenate([ends_a_ref[...], ends_b], axis=0)
    size = pairs * heads

    def pair_of(index):
        position = index // heads
        offset = position * 0
        for p in range(pairs):
            offset = jnp.where(position == p, offsets[p], offset)
        return (span ^ offset) >> 1, index % heads

    mine, my_head = pair_of(iota2((size, size), 0))
    other, other_head = pair_of(iota2((size, size), 1))
    between = (other > mine) & (other < (span >> 1)) & (my_head == other_head)
    carried = exact_dot(between.astype(F32), ends)
    before = jnp.where(odd_span, before_ref[...], 0.0)
    factor = jnp.exp(carried + jnp.concatenate([before] * pairs, axis=0))
    early_at = {offset: i for i, (offset, _) in enumerate(early_table)}
    late_at = {offset: i for i, (offset, _) in enumerate(late_table)}
    bases = {i: early_at[offset] for i, (offset, _) in enumerate(late_table) if offset in early_at}

    def sum_level(level):
        chosen = [k for k in sorted({*early_at, *late_at}) if max(k, 1).bit_length() - 1 == level]
        for h in range(heads):
            value = None
            for k in chosen:
                state = state_scr[late_at[k], h] if k in late_at else state_a_ref[early_at[k], h]
                if k:
                    at = offsets.index(k) * heads + h
                    state = state * factor[at : at + 1, :]
                value = state if value is None else value + state
            level_state_ref[level, h] = value

    peak_scr[...] = peak_a_ref[...]
    late_levels = dict(by_level(late_table))
    for level in range(span_bits):
        used = ((span >> level) & 1) == 1

        @pl.when(used)
        def _(level=level):
            if level in late_levels:
                take_level(
                    late_levels[level], q_all, *late_refs, weights, score_scr, peak_scr, state_scr, state_a_ref, bases
                )
            sum_level(level)

        @pl.when(jnp.logical_not(used))
        def _(level=level):
            level_state_ref[level] = jnp.zeros_like(level_state_ref[level])

    peak = jnp.max(peak_scr[...], axis=1, keepdims=True)
    peak_scr[...] = jnp.broadcast_to(peak, peak_scr.shape)

    def weigh(early_units, late_units):
        top = peak_scr[...]
        total, parts, values = None, [], []
        for units, refs, score_ref in ((early_units, early_refs, score_a_ref), (late_units, late_refs, score_scr)):
            for part, p in units:
                weight = jnp.exp2(score_ref[part * count + p] - top)
                total = weight if total is None else total + weight
                parts.append(weight.astype(BF16))
                values += unit_values(refs[0][part], refs[1][part], p)
        return total, dot(jnp.concatenate(parts, axis=1), jnp.concatenate(values, axis=0))

    total_scr[...], acc_scr[...] = weigh([(0, 0), (1, 0)], [])
    early_levels = dict(by_level(early_table))
    for bit in sorted({*early_levels, *late_levels}):

        @pl.when(((span >> bit) & 1) == 1)
        def _(bit=bit):
            total, acc = weigh(
                [unit for _, units in early_levels.get(bit, []) for unit in units],
                [unit for _, units in late_levels.get(bit, []) for unit in units],
            )
            total_scr[...] += total
            acc_scr[...] += acc

    total = jnp.sum(total_scr[...], axis=1, keepdims=True)
    target_all = acc_scr[...] / total
    combined = []
    for h in range(heads):
        value = level_ref[h, low_bits + 1] * level_state_ref[0, h]
        for level in range(1, span_bits):
            value = value + level_ref[h, low_bits + 1 + level] * level_state_ref[level, h]
        value = halves(value)
        comb_ref[h, 0], comb_ref[h, 1] = value
        combined.append(value)
    fars = [dot_f32((qe_ref[h, 0], qe_ref[h, 1]), combined[h]) for h in range(heads)]
    squares = jnp.zeros((rows, dim), F32)
    gained = jnp.zeros((rows, dim), F32)
    crossed = jnp.zeros((rows, dim), F32)
    for h in range(heads):
        raw = loc_ref[h] + fars[h]
        target = target_all[h * rows : (h + 1) * rows]
        raw_ref[h] = raw
        target_ref[h] = target
        gain = gain_ref[h : h + 1, :]
        square = raw * raw
        squares = squares + square
        gained = gained + square * (gain * gain)
        crossed = crossed + target * raw * gain
    lanes = iota2((rows, rows), 1)
    columns = jnp.where(
        lanes == 0,
        jnp.sum(squares, axis=1, keepdims=True),
        jnp.where(
            lanes == 1,
            jnp.sum(gained, axis=1, keepdims=True),
            jnp.where(lanes == 2, jnp.sum(crossed, axis=1, keepdims=True), 0.0),
        ),
    )
    sums_ref[...] = columns.T[0:8]


def chunk_of(head, heads, span, splits):
    group = heads >> len(splits)
    chunk = 0
    for place, stride in enumerate(splits):
        shift = len(splits) - 1 - place
        bit = (head // group >> shift) & 1
        chunk = chunk + ((bit ^ ((span // stride) & 1)) << shift)
    return chunk * group + head % group


def backward_kernel(
    span_ref, sums_a_ref, sums_b_ref, entry_ref, q_ref, k_ref, v_ref, gain_ref,
    qp_ref, qe_ref, km_ref, sd_ref, mix_ref, raw_ref, target_ref, state_ref, comb_ref,
    keep_ref, send_ref, *, norm_width, total_tokens, splits, heads,
):
    _, rows, dim = raw_ref.shape
    share = len(heads)
    span_bits = state_ref.shape[0]
    low_bits = rows.bit_length() - 1
    span = span_ref[0]
    first = (span & 1) == 0
    sums = (sums_a_ref[...] + sums_b_ref[...]).T
    squares, gained, crossed = sums[:, 0:1], sums[:, 1:2], sums[:, 2:3]
    inverse = lax.rsqrt(squares / norm_width + EPSILON)
    inner = (inverse * gained - crossed) / total_tokens
    shrink = inverse * inverse * inverse * inner / norm_width
    levels = low_bits + 1 + span_bits
    pad = 16
    gain_rows, residuals, highs, lows = [], [], [], []
    for h in heads:
        gain = gain_ref[h : h + 1, :]
        raw = raw_ref[h]
        normed = raw * inverse
        mismatch = (normed * gain - target_ref[h]) * (1.0 / total_tokens)
        gain_rows.append(jnp.sum(mismatch * normed, axis=0, keepdims=True))
        residual = inverse * (mismatch * gain) - raw * shrink
        residuals.append(residual)
        high, low = halves(residual)
        highs.append(high)
        lows.append(low)
    d_mix = dot_left((jnp.concatenate(highs, axis=0), jnp.concatenate(lows, axis=0)), v_ref[...], NT)
    leads = [halves(entry_ref[:, h : h + 1] * residual) for h, residual in zip(heads, residuals)]
    d_fars = [dot_f32(lead, (comb_ref[h, 0], comb_ref[h, 1]), NT) for h, lead in zip(heads, leads)]
    d_combs = [
        dot_f32((qe_ref[h, 0], qe_ref[h, 1]), (high, low), TN) for h, high, low in zip(heads, highs, lows)
    ]
    throughs, highs, lows = [], [], []
    for i, h in enumerate(heads):
        d_mix_h = d_mix[i * rows : (i + 1) * rows]
        high, low = halves(d_mix_h * mix_ref[h])
        highs.append(high)
        lows.append(low)
        throughs.append(d_mix_h * sd_ref[h])
    d_local = dot_left((jnp.concatenate(highs, axis=0), jnp.concatenate(lows, axis=0)), k_ref[...])
    d_qts = [halves(d_local[i * rows : (i + 1) * rows] + d_fars[i]) for i in range(share)]
    d_qps = [halves(dot_f32(d_qts[i], (km_ref[h, 0], km_ref[h, 1]))) for i, h in enumerate(heads)]
    grads_k = [dot_f32(d_qts[i], (qp_ref[h, 0], qp_ref[h, 1]), TN) for i, h in enumerate(heads)]
    grads_q = [dot_right(q_ref[h * rows : (h + 1) * rows, :], d_qps[i], TN) for i, h in enumerate(heads)]

    block = 8
    inside = block.bit_length() - 1
    lane = iota2((block, rows), 1)
    near = iota2((block, rows), 0) ^ (lane % block)
    apart = [(lane // block) ^ i for i in range(rows // block)]
    level_rows = []
    for i, h in enumerate(heads):
        pieces = [throughs[i][at : at + block] for at in range(0, rows, block)]
        sums_by = [jnp.zeros((block, rows), F32) for _ in range(low_bits + 1 - inside)]
        for piece, distance in zip(pieces, apart):
            for level in range(len(sums_by)):
                here = distance == 0 if level == 0 else (distance >> (level - 1)) == 1
                sums_by[level] = sums_by[level] + jnp.where(here, piece, 0.0)
        for level in range(inside + 1):
            here = near == 0 if level == 0 else (near >> (level - 1)) == 1
            level_rows.append(jnp.sum(jnp.where(here, sums_by[0], 0.0), axis=0, keepdims=True))
        for level in range(1, len(sums_by)):
            level_rows.append(jnp.sum(sums_by[level], axis=0, keepdims=True))
        for level in range(span_bits):
            level_rows.append(jnp.sum(state_ref[level, h] * d_combs[i], axis=0, keepdims=True))
        level_rows.append(jnp.zeros((pad - levels, rows), F32))
    for i in range(share):
        at = pl.ds(pl.multiple_of(chunk_of(i, share, span, splits) * dim, dim), dim)
        keep_ref[at, :] = jnp.where(first, grads_q[i], grads_k[i])
        send_ref[at, :] = jnp.where(first, grads_k[i], grads_q[i])
    table = jnp.sum(jnp.concatenate(level_rows, axis=0), axis=1, keepdims=True)
    spread = iota2((share * pad, rows), 0) % pad == iota2((share * pad, rows), 1)
    pick = iota2((share, share * pad), 1) // pad == iota2((share, share * pad), 0)
    level_sums = exact_dot(pick.astype(F32), jnp.where(spread, table, 0.0))
    small = jnp.concatenate(gain_rows + [level_sums], axis=0)
    tail = pl.ds(share * dim, 2 * share)
    keep_ref[tail, :] = small
    send_ref[tail, :] = small


def place_kernel(span_ref, *refs, orders):
    q_ref, k_ref, level_ref, gain_ref = refs[-4:]
    heads, dim, _ = q_ref.shape
    parts = len(orders)
    share = heads // parts
    span = span_ref[0]
    first = (span & 1) == 0
    for part, splits in enumerate(orders):
        mine_ref, other_ref, small_ref = refs[3 * part : 3 * part + 3]
        tail = small_ref.shape[0] - 2 * share
        for i in range(share):
            h = part * share + i
            at = pl.ds(pl.multiple_of(chunk_of(i, share, span, splits) * dim, dim), dim)
            mine, other = mine_ref[at, :], other_ref[at, :]
            q_ref[h] = jnp.where(first, mine, other)
            k_ref[h] = jnp.where(first, other, mine)
        heads_here = pl.ds(part * share, share)
        gain_ref[heads_here, :] = small_ref[tail : tail + share, :]
        level_ref[heads_here, :] = small_ref[tail + share :, : level_ref.shape[1]]


def vmem(count):
    return [pl.BlockSpec(memory_space=pltpu.VMEM)] * count


def hbm(count):
    return [pl.BlockSpec(memory_space=pltpu.HBM)] * count


def smem(count):
    return [pl.BlockSpec(memory_space=pltpu.SMEM)] * count


def shape(*dims, dtype=F32):
    return jax.ShapeDtypeStruct(dims, dtype)


def call(kernel, ins, outs, limit, flops, scratch=(), **static):
    body = functools.partial(kernel, **static) if static else kernel
    single = not isinstance(outs, (list, tuple))
    return pl.pallas_call(
        body,
        out_shape=outs,
        in_specs=ins,
        out_specs=pl.BlockSpec(memory_space=pltpu.VMEM) if single else vmem(len(outs)),
        scratch_shapes=list(scratch),
        compiler_params=pltpu.CompilerParams(vmem_limit_bytes=limit << 20),
        cost_estimate=pl.CostEstimate(flops=flops, bytes_accessed=1 << 20, transcendentals=0),
    )


def in_hbm(*values):
    return [pltpu.with_memory_space_constraint(value, pltpu.HBM) for value in values]


def swap(value, axis, stride):
    count = lax.axis_size(axis)
    return lax.ppermute(value, axis, [(i, i ^ stride) for i in range(count)])


def on_device(queries, key_vectors, value_vectors, log_gate, query_map, key_map, level_weight, norm_gain):
    rows, dim = key_vectors.shape
    heads = queries.shape[1] // dim
    count = lax.axis_size("seq")
    groups = lax.axis_size("head")
    span_bits = count.bit_length() - 1
    span = lax.axis_index("seq").astype(jnp.int32).reshape(1)
    total_tokens = rows * count
    norm_width = heads * dim * groups
    gain = norm_gain.reshape(heads, dim)
    strides = [1 << bit for bit in reversed(range(1, span_bits))]
    orders = [(2, 4), (4, 2)]
    cube = (heads, dim, dim)
    pieces = shape(heads, 2, rows, dim, dtype=BF16)
    packed_rows = rows + 3 * heads

    shared, (far, near) = strides[:-2], strides[-2:]
    offsets = [0]
    for stride in shared:
        offsets += [offset + stride for offset in offsets]
    early = [offsets + [offset + turn for offset in offsets] for turn in (far, near)]
    late = [[offset + turn for offset in row] for row, turn in zip(early, (near, far))]
    count_early = len(early[0])

    packed = call(pack_kernel, hbm(3), shape(2, 1, packed_rows, dim, dtype=BF16), 8, 1 << 20, scratch=[
        pltpu.VMEM((rows, dim), BF16),
        pltpu.VMEM((rows, dim), BF16),
        pltpu.VMEM((heads, rows), F32),
        pltpu.SemaphoreType.DMA((3,)),
    ])(*in_hbm(key_vectors, value_vectors, log_gate))
    qp, qe, km, score_decay, mix, local, entry, stacked = call(
        local_kernel, vmem(1) + hbm(4), [pieces] * 3 + [shape(*cube)] * 3 + [shape(rows, heads), shape(heads * rows, dim, dtype=BF16)], 24, 1 << 29,
        scratch=[
            pltpu.VMEM(queries.shape, BF16),
            pltpu.VMEM(cube, F32),
            pltpu.VMEM(cube, F32),
            pltpu.SMEM(level_weight.shape, F32),
            pltpu.SemaphoreType.DMA((4,)),
        ],
    )(packed, *in_hbm(level_weight, queries, query_map, key_map))

    held = packed
    for stride in shared:
        received = swap(held, "seq", stride)
        held = jnp.concatenate([held, received], axis=1)
    evens, odds = [], []
    for part, turn in enumerate((far, near)):
        evens.append(jnp.concatenate([held[part], swap(held[part], "seq", turn)], axis=0))
    for part, turn in enumerate((near, far)):
        evens.append(swap(evens[part], "seq", turn))
        odds.append(swap(evens[part], "seq", 1))
    for part in range(2):
        odds.append(swap(evens[2 + part], "seq", 1))
    blocks = [value for pair in zip(evens, odds) for value in pair]

    scores, peaks, states, ends, before = call(
        early_kernel,
        smem(1) + vmem(5),
        [
            shape(2 * count_early, heads * rows, rows),
            shape(heads * rows, rows),
            shape(len(pairs_of(early)), *cube),
            shape(count_early * heads, rows),
            shape(heads, rows),
        ],
        24,
        1 << 30,
        offsets=early,
    )(span, stacked, *blocks[:4])
    raw, target, level_states, combined, sums = call(
        forward_kernel,
        smem(2) + vmem(17),
        [shape(*cube), shape(*cube), shape(span_bits, *cube), pieces, shape(8, rows)],
        32,
        1 << 31,
        scratch=[
            pltpu.VMEM((2 * count_early, heads * rows, rows), F32),
            pltpu.VMEM((heads * rows, rows), F32),
            pltpu.VMEM((len(pairs_of(late)), *cube), F32),
            pltpu.VMEM((heads * rows, rows), F32),
            pltpu.VMEM((heads * rows, dim), F32),
        ],
        early=early,
        late=late,
    )(
        span, level_weight, stacked, *blocks, scores, peaks, states, ends, before, qe, local, gain,
    )

    stride = 1
    while stride < groups:
        received = swap(sums, "head", stride)
        if 2 * stride < groups:
            sums = sums + received
        stride *= 2

    share = heads // PARTS
    size = share * dim
    held = []
    for part in range(PARTS):
        keep, send = call(
            backward_kernel,
            smem(1) + vmem(16),
            [shape(share * (dim + 2), dim)] * 2,
            24,
            1 << 29,
            norm_width=float(norm_width),
            total_tokens=float(total_tokens),
            splits=orders[part],
            heads=range(part * share, (part + 1) * share),
        )(
            span, sums, received, entry, stacked, key_vectors, value_vectors, gain,
            qp, qe, km, score_decay, mix, raw, target, level_states, combined,
        )
        held.append(keep + swap(send, "seq", 1))
    for step in range(len(orders[0])):
        size //= 2
        for part in range(PARTS):
            split = orders[part][step]
            here = held[part]
            got = swap(here[size:], "seq", split)
            held[part] = jnp.concatenate([here[:size] + got[:size], here[2 * size :] + got[size:]])
    for stride in strides:
        if stride not in orders[0]:
            for part in range(PARTS):
                held[part] = held[part] + swap(held[part], "seq", stride)
    mine = [here[:size] for here in held]
    for step in reversed(range(len(orders[0]))):
        for part in range(PARTS):
            split = orders[part][step]
            mine[part] = jnp.concatenate([mine[part], swap(mine[part], "seq", split)])
    found = []
    for part in range(PARTS):
        found += [mine[part], swap(mine[part], "seq", 1), held[part]]
    grad_query, grad_key, grad_levels, grad_gain = call(
        place_kernel,
        smem(1) + vmem(3 * PARTS),
        [shape(*cube), shape(*cube), shape(*level_weight.shape), shape(heads, dim)],
        16,
        1 << 20,
        orders=orders,
    )(span, *found)
    grad_gain = grad_gain.reshape(-1)
    return grad_query, grad_key, grad_levels, grad_gain


def solution(mesh):
    placed = (
        P("seq", "head"),
        P("seq", "head"),
        P("seq", "head"),
        P("head", "seq"),
        P("head", None, None),
        P("head", None, None),
        P("head", None),
        P("head"),
    )

    return jax.shard_map(
        on_device,
        mesh=mesh,
        in_specs=placed,
        out_specs=(P("head", None, None), P("head", None, None), P("head", None), P("head")),
        check_vma=False,
    )
```
